256 devices in a mesh: depth: 32 (over z, x_lo, core), band: 8 (over y, x_hi).
Axes of the slice: x: 4 (x_hi: 2, x_lo: 2; x = x_hi * 2 + x_lo), y: 4, z: 8, core: 2. Of those that a mesh axis runs over, the one named last changes fastest.
Arguments:
- volume: int32 [128, 256, 1024], P('depth', 'band'), may hold values from 0 to 255
- tf_table: int32 [4, 256], replicated, may hold values from 0 to 255
- view_code: int32 [2, 4], replicated, may hold values from -20 to 20
Outputs:
- final_image: float32 [2, 1024, 4, 256], P(None, 'depth', None, 'band')
The draws below stay inside these ranges and needn't reach their ends.
All inputs are finite; a program needn't handle non-finite values.
Results may differ from the reference program's by a relative error of at most 0.0014.
Values may be sent and summed in bfloat16 or wider, within the bound.
No kernel may reach another device: no remote copies, remote signals or barrier semaphores. Data moves between devices by JAX's collectives and lax.ppermute only.
A program may use at most 64 MiB of HBM per device.

```python
import jax
import jax.numpy as jnp
from jax import lax

NX = 1024
VIEWS = 2
LEVELS = 256
QMAX = 20
MARGIN = 16
NY = 256
NZ = 128


def place_ends(values, stream_key, low, high):
    index_at = [jax.random.randint(jax.random.fold_in(stream_key, axis), (), 0, length) for axis, length in enumerate(values.shape)]
    widest = values.shape.index(max(values.shape))
    next_to = index_at[:widest] + [(index_at[widest] + 1) % values.shape[widest]] + index_at[widest + 1:]
    return values.at[tuple(index_at)].set(low).at[tuple(next_to)].set(high)


def setup_inputs(seed: int = 0) -> dict:
    seeds = jax.random.split(jax.random.key(seed), 4)
    return {
        "volume": place_ends(jax.random.randint(seeds[0], (NZ, NY, NX), 0, LEVELS), jax.random.fold_in(seeds[0], 1), 0, LEVELS - 1).astype(jnp.int32),
        "tf_table": place_ends(jax.random.randint(seeds[1], (4, LEVELS), 0, 256), jax.random.fold_in(seeds[1], 1), 0, 255).astype(jnp.int32),
        "view_code": place_ends(jax.random.randint(seeds[2], (VIEWS, 4), -QMAX, QMAX + 1), jax.random.fold_in(seeds[2], 1), -QMAX, QMAX).astype(jnp.int32),
    }


tap_steps = (-2, -1, 0, 1, 2, 3)


def lanczos(offset):
    return jnp.where(jnp.abs(offset) < 3.0, jnp.sinc(offset) * jnp.sinc(offset / 3.0), 0.0)


def split_offset(coefficient, position, length, lift=0):
    numerator = coefficient * (2 * position + 1 - length) + lift * length
    integer_part = (numerator // (2 * length)).astype(jnp.int32)
    fraction = (numerator - integer_part * (2 * length)).astype(jnp.float32) / (2.0 * length)
    return integer_part, fraction


def make_palette(tf_table, depth_count):
    table_float = tf_table.astype(jnp.float32)
    opacity = table_float[3] / (64.0 * depth_count)
    premult = table_float[0:3] / 255.0 * opacity
    return jnp.concatenate([premult, opacity[None]], axis=0).astype(jnp.bfloat16)


def shear_taps(source, integer_part, fraction, along, margin):
    extent = source.shape[along]
    widths = [(0, 0)] * source.ndim
    widths[along] = (margin, margin)
    padded = jnp.pad(source.astype(jnp.float32), widths)
    accumulated = jnp.zeros(source.shape, jnp.float32)
    for step_value in tap_steps:
        tap_weight = lax.optimization_barrier(lanczos(fraction - step_value).astype(jnp.bfloat16))
        start = (margin + integer_part + step_value).astype(jnp.int32)
        shifted = lax.dynamic_slice_in_dim(padded, start, extent, along)
        accumulated = accumulated + tap_weight.astype(jnp.float32) * shifted
    return accumulated


def render(volume, palette, params):
    facing = params[3] >= 0

    def advance(picture, slice_step):
        depth_index = jnp.where(facing, slice_step, NZ - 1 - slice_step).astype(jnp.int32)
        voxels = lax.dynamic_index_in_dim(volume, depth_index, 0, keepdims=False)
        classified = jnp.take(palette, voxels, axis=1)
        whole_x, frac_x = split_offset(params[0], depth_index, NZ)
        whole_y, frac_y = split_offset(params[1], depth_index, NZ)
        row_sheared = shear_taps(classified, whole_x, frac_x, 2, MARGIN).astype(jnp.bfloat16)
        row_sheared = lax.optimization_barrier(row_sheared)
        sheared = shear_taps(row_sheared, whole_y, frac_y, 1, MARGIN)
        return picture + (1.0 - picture[3:4]) * sheared, None

    start_picture = jnp.zeros((4, NY, NX), jnp.float32)
    picture, unused = lax.scan(advance, start_picture, jnp.arange(NZ, dtype=jnp.int32))
    return picture


def warp_columns(picture, coefficient):
    columns = jnp.arange(NX, dtype=jnp.int32)
    integer_part, fraction = split_offset(coefficient, columns, NX, 1)
    accumulated = jnp.zeros(picture.shape, jnp.float32)
    for step_value in tap_steps:
        tap_weight = lanczos(fraction - step_value)
        source_index = (columns + integer_part + step_value).astype(jnp.int32)
        inside = (source_index >= 0) & (source_index < NX)
        picked = jnp.take(picture, jnp.clip(source_index, 0, NX - 1), axis=2)
        accumulated = accumulated + jnp.where(inside, tap_weight, 0.0) * picked
    return jnp.transpose(accumulated, (2, 0, 1))


def reference(volume, tf_table, view_code):
    palette = make_palette(tf_table, NZ)
    finals = []
    for view_index in range(VIEWS):
        params = view_code[view_index]
        picture = render(volume, palette, params)
        finals.append(warp_columns(picture, params[2]))
    return jnp.stack(finals)
```

```python
import jax
import jax.numpy as jnp
from jax import lax
from jax.experimental import pallas as pl
from jax.experimental.pallas import tpu as pltpu
from jax.sharding import PartitionSpec as P

VIEWS = 2
HALO = 16
LANES = 128
CENTER = 64


def sinc(t):
    angle = jnp.where(t == 0.0, 1.0, jnp.pi * t)
    return jnp.where(t == 0.0, 1.0, jnp.sin(angle) / angle)


def lanczos(offset):
    return jnp.where(jnp.abs(offset) < 3.0, sinc(offset) * sinc(offset / 3.0), 0.0)


def iota(shape, dim):
    return lax.broadcasted_iota(jnp.int32, shape, dim)


def pairs(size, first):
    out = []
    for a in range(first, size - 1, 2):
        out += [(a, a + 1), (a + 1, a)]
    return out


def lane_pick(row, index):
    table = jnp.broadcast_to(row, index.shape)
    return jnp.take_along_axis(table, index, axis=1, mode="promise_in_bounds")


def shear_kernel(ids, view, tf, vol, got_a, got_b, out, classed, moved, picture):
    slab, rows, width = vol.shape
    blocks = width // LANES
    wide = rows + 2 * HALO
    depth_rank, band_rank = ids[0], ids[1]
    depth = slab * ids[2]
    height = rows * ids[3]

    codes = tf[...].astype(jnp.float32)
    opacity = codes[3:4] / (64.0 * depth.astype(jnp.float32))
    premult = codes[0:3] / 255.0 * opacity
    palette = jnp.concatenate([premult, opacity], axis=0).astype(jnp.bfloat16).astype(jnp.float32)

    which = iota((VIEWS * slab, LANES), 0)
    lane = iota((VIEWS * slab, LANES), 1)
    place = depth_rank * slab + which % slab
    taps = []
    for column in range(2):
        q = jnp.where(which < slab, view[0, column], view[1, column])
        num = q * (2 * place + 1 - depth)
        whole = num // (2 * depth)
        frac = (num - whole * (2 * depth)).astype(jnp.float32) / (2.0 * depth.astype(jnp.float32))
        taps.append(
            lanczos(frac - (lane - CENTER).astype(jnp.float32))
            .astype(jnp.bfloat16)
            .astype(jnp.float32)
        )

    def shift(v, s, column):
        num = view[v, column] * (2 * (depth_rank * slab + s) + 1 - depth)
        return num // (2 * depth)

    base_x = iota((2 * LANES, LANES), 0) - iota((2 * LANES, LANES), 1)
    shape_y = (4 * rows, 4 * wide)
    to = iota(shape_y, 0)
    frm = iota(shape_y, 1)
    even = band_rank % 2 == 0
    start_a = jnp.where(even, rows, -HALO)
    start_b = jnp.where(even, -HALO, rows)
    at = frm % wide
    local = jnp.where(
        at < rows,
        at,
        jnp.where(at < rows + HALO, at - rows + start_a, at - rows - HALO + start_b),
    )
    world = local + band_rank * rows
    fits = (to // rows == frm // wide) & (world >= 0) & (world < height)
    base_y = jnp.where(fits, local - to % rows + CENTER, -4 * LANES)

    for s in range(slab):
        voxels = jnp.concatenate(
            [vol[s], got_a[s].astype(jnp.int32), got_b[s].astype(jnp.int32)], axis=0
        )
        side = jnp.zeros((wide, CENTER), jnp.int32)
        voxels = jnp.concatenate([side, voxels, side], axis=1)
        for k in range(blocks + 1):
            code = voxels[:, k * LANES : (k + 1) * LANES]
            high = code >= LANES
            low = code & (LANES - 1)
            for c in range(4):
                value = jnp.where(
                    high,
                    lane_pick(palette[c : c + 1, LANES:], low),
                    lane_pick(palette[c : c + 1, :LANES], low),
                )
                if k == 0:
                    value = jnp.where(iota(value.shape, 1) >= CENTER, value, 0.0)
                if k == blocks:
                    value = jnp.where(iota(value.shape, 1) < CENTER, value, 0.0)
                classed[c * wide : (c + 1) * wide, k * LANES : (k + 1) * LANES] = value.astype(
                    jnp.bfloat16
                )
        weights = jnp.concatenate(
            [
                lane_pick(
                    taps[0][v * slab + s : v * slab + s + 1],
                    jnp.clip(base_x - shift(v, s, 0), 0, LANES - 1),
                ).astype(jnp.bfloat16)
                for v in range(VIEWS)
            ],
            axis=1,
        )
        for k in range(blocks):
            part = jnp.dot(
                classed[:, k * LANES : (k + 2) * LANES],
                weights,
                preferred_element_type=jnp.float32,
            ).astype(jnp.bfloat16)
            for v in range(VIEWS):
                moved[v, :, k * LANES : (k + 1) * LANES] = part[:, v * LANES : (v + 1) * LANES]
        for v in range(VIEWS):
            index = jnp.clip(base_y - shift(v, s, 1), 0, LANES - 1)
            row = taps[1][v * slab + s : v * slab + s + 1]
            weights = jnp.concatenate(
                [
                    lane_pick(row, index[:, j * LANES : (j + 1) * LANES]).astype(jnp.bfloat16)
                    for j in range(4 * wide // LANES)
                ],
                axis=1,
            )
            facing = view[v, 3] >= 0
            for k in range(0, width, 256):
                sheared = jnp.dot(
                    weights, moved[v, :, k : k + 256], preferred_element_type=jnp.float32
                )
                if s == 0:
                    picture[v, :, k : k + 256] = sheared
                    continue
                before = picture[v, :, k : k + 256]
                front = jnp.where(facing, before, sheared)
                back = jnp.where(facing, sheared, before)
                through = 1.0 - front[3 * rows :]
                picture[v, :, k : k + 256] = front + jnp.concatenate([through] * 4, axis=0) * back
    strips = out.shape[0]
    strip = width // strips
    for v in range(VIEWS):
        for k in range(blocks):
            turned = picture[v, :, k * LANES : (k + 1) * LANES].T.astype(jnp.bfloat16)
            per = LANES // strip
            out[k * per : (k + 1) * per, v * strip : (v + 1) * strip, :] = turned.reshape(
                per, strip, 4 * rows
            )


def gather_kernel(ids, view, arrived, strip_out, send_a, send_b):
    slabs, both, lanes = arrived.shape
    strip = both // VIEWS
    rows = lanes // 4
    pick = 3 * rows + iota((strip, lanes), 1) % rows
    even = ids[0] % 2 == 0
    for v in range(VIEWS):
        facing = view[v, 3] >= 0
        picture = jnp.zeros((strip, lanes), jnp.float32)
        through = jnp.ones((strip, lanes), jnp.float32)
        for k in range(slabs):
            at = jnp.where(facing, k, slabs - 1 - k)
            part = arrived[at, v * strip : (v + 1) * strip, :].astype(jnp.float32)
            picture = picture + through * part
            through = through * (
                1.0 - jnp.take_along_axis(part, pick, axis=1, mode="promise_in_bounds")
            )
        strip_out[v] = picture
        first = picture[:HALO]
        last = picture[strip - HALO :]
        send_a[v] = jnp.where(even, last, first)
        send_b[v] = jnp.where(even, first, last)


def warp_kernel(ids, view, strip_in, got_a, got_b, out):
    strip, lanes = strip_in.shape[1:]
    width = strip * ids[2]
    even = ids[0] % 2 == 0
    shape = (strip, strip + 2 * HALO)
    start_a = jnp.where(even, strip, -HALO)
    start_b = jnp.where(even, -HALO, strip)
    at = iota(shape, 1)
    local = jnp.where(
        at < strip,
        at,
        jnp.where(at < strip + HALO, at - strip + start_a, at - strip - HALO + start_b),
    )
    column = iota(shape, 0)
    for v in range(VIEWS):
        num = view[v, 2] * (2 * (ids[0] * strip + column) + 1 - width) + width
        whole = num // (2 * width)
        frac = (num - whole * (2 * width)).astype(jnp.float32) / (2.0 * width.astype(jnp.float32))
        weights = lanczos(frac - (local - column - whole).astype(jnp.float32))
        source = jnp.concatenate([strip_in[v], got_a[v], got_b[v]], axis=0)
        out[v] = jnp.dot(
            weights,
            source,
            precision=lax.Precision.HIGHEST,
            preferred_element_type=jnp.float32,
        )


def call(kernel, outs, scratch=(), vmem_from=2):
    def run(*args):
        return pl.pallas_call(
            kernel,
            out_shape=outs,
            in_specs=[pl.BlockSpec(memory_space=pltpu.SMEM)] * vmem_from
            + [pl.BlockSpec(memory_space=pltpu.VMEM)] * (len(args) - vmem_from),
            out_specs=jax.tree.map(lambda _: pl.BlockSpec(memory_space=pltpu.VMEM), outs),
            scratch_shapes=list(scratch),
        )(*args)

    return run


def body(volume, tf_table, view_code):
    slab, rows, width = volume.shape
    depth_size = lax.axis_size("depth")
    band_size = lax.axis_size("band")
    depth_rank = lax.axis_index("depth")
    band_rank = lax.axis_index("band")
    strip = width // depth_size
    wide = rows + 2 * HALO
    lanes = 4 * rows
    ids = jnp.stack(
        [depth_rank, band_rank, jnp.int32(depth_size), jnp.int32(band_size)]
    ).astype(jnp.int32)
    even = band_rank % 2 == 0
    first = volume[:, :HALO]
    last = volume[:, rows - HALO :]
    got_a = lax.ppermute(
        jnp.where(even, last, first).astype(jnp.bfloat16), "band", pairs(band_size, 0)
    )
    got_b = lax.ppermute(
        jnp.where(even, first, last).astype(jnp.bfloat16), "band", pairs(band_size, 1)
    )
    pieces = call(
        shear_kernel,
        jax.ShapeDtypeStruct((depth_size, VIEWS * strip, lanes), jnp.bfloat16),
        (
            pltpu.VMEM((4 * wide, width + LANES), jnp.bfloat16),
            pltpu.VMEM((VIEWS, 4 * wide, width), jnp.bfloat16),
            pltpu.VMEM((VIEWS, lanes, width), jnp.float32),
        ),
    )(ids, view_code, tf_table, volume, got_a, got_b)
    arrived = lax.all_to_all(pieces, "depth", split_axis=0, concat_axis=0, tiled=True)
    edge = jax.ShapeDtypeStruct((VIEWS, HALO, lanes), jnp.float32)
    whole = jax.ShapeDtypeStruct((VIEWS, strip, lanes), jnp.float32)
    middle, send_a, send_b = call(gather_kernel, (whole, edge, edge))(ids, view_code, arrived)
    side_a = lax.ppermute(send_a, "depth", pairs(depth_size, 0))
    side_b = lax.ppermute(send_b, "depth", pairs(depth_size, 1))
    final = call(warp_kernel, whole)(ids, view_code, middle, side_a, side_b)
    return final.reshape(VIEWS, strip, 4, rows)


def solution(mesh):
    placed = (P("depth", "band", None), P(), P())
    return jax.shard_map(
        body, mesh=mesh, in_specs=placed, out_specs=P(None, "depth", None, "band"), check_vma=False
    )
```

```python
import jax
import jax.numpy as jnp
from jax import lax
from jax.experimental import pallas as pl
from jax.experimental.pallas import tpu as pltpu
from jax.sharding import PartitionSpec as P

VIEWS = 2
HALO = 16
LANES = 128
CENTER = 64
VMEM_LIMIT = 16 * 2**20


def sinc(t):
    angle = jnp.where(t == 0.0, 1.0, jnp.pi * t)
    return jnp.where(t == 0.0, 1.0, jnp.sin(angle) / angle)


def lanczos(offset):
    return jnp.where(jnp.abs(offset) < 3.0, sinc(offset) * sinc(offset / 3.0), 0.0)


def iota(shape, dim):
    return lax.broadcasted_iota(jnp.int32, shape, dim)


def pairs(size, first):
    out = []
    for a in range(first, size - 1, 2):
        out += [(a, a + 1), (a + 1, a)]
    return out


def lane_pick(row, index):
    table = jnp.broadcast_to(row, index.shape)
    return jnp.take_along_axis(table, index, axis=1, mode="promise_in_bounds")


def shear_kernel(ids, view, tf, vol, got_a, got_b, out, classed, moved, picture):
    slab, rows, width = vol.shape
    blocks = width // LANES
    wide = rows + 2 * HALO
    depth_rank, band_rank = ids[0], ids[1]
    depth = slab * ids[2]
    height = rows * ids[3]

    codes = tf[...].astype(jnp.float32)
    opacity = codes[3:4] / (64.0 * depth.astype(jnp.float32))
    premult = codes[0:3] / 255.0 * opacity
    palette = jnp.concatenate([premult, opacity], axis=0).astype(jnp.bfloat16).astype(jnp.float32)

    which = iota((VIEWS * slab, LANES), 0)
    lane = iota((VIEWS * slab, LANES), 1)
    place = depth_rank * slab + which % slab
    taps = []
    for column in range(2):
        q = jnp.where(which < slab, view[0, column], view[1, column])
        num = q * (2 * place + 1 - depth)
        whole = num // (2 * depth)
        frac = (num - whole * (2 * depth)).astype(jnp.float32) / (2.0 * depth.astype(jnp.float32))
        taps.append(
            lanczos(frac - (lane - CENTER).astype(jnp.float32))
            .astype(jnp.bfloat16)
            .astype(jnp.float32)
        )

    def shift(v, s, column):
        num = view[v, column] * (2 * (depth_rank * slab + s) + 1 - depth)
        return num // (2 * depth)

    base_x = iota((2 * LANES, LANES), 0) - iota((2 * LANES, LANES), 1)
    shape_y = (4 * rows, 4 * wide)
    to = iota(shape_y, 0)
    frm = iota(shape_y, 1)
    even = band_rank % 2 == 0
    start_a = jnp.where(even, rows, -HALO)
    start_b = jnp.where(even, -HALO, rows)
    at = frm % wide
    local = jnp.where(
        at < rows,
        at,
        jnp.where(at < rows + HALO, at - rows + start_a, at - rows - HALO + start_b),
    )
    world = local + band_rank * rows
    fits = (to // rows == frm // wide) & (world >= 0) & (world < height)
    base_y = jnp.where(fits, local - to % rows + CENTER, -4 * LANES)

    for s in range(slab):
        voxels = jnp.concatenate(
            [vol[s], got_a[s].astype(jnp.int32), got_b[s].astype(jnp.int32)], axis=0
        )
        side = jnp.zeros((wide, CENTER), jnp.int32)
        voxels = jnp.concatenate([side, voxels, side], axis=1)
        for k in range(blocks + 1):
            code = voxels[:, k * LANES : (k + 1) * LANES]
            high = code >= LANES
            low = code & (LANES - 1)
            for c in range(4):
                value = jnp.where(
                    high,
                    lane_pick(palette[c : c + 1, LANES:], low),
                    lane_pick(palette[c : c + 1, :LANES], low),
                )
                if k == 0:
                    value = jnp.where(iota(value.shape, 1) >= CENTER, value, 0.0)
                if k == blocks:
                    value = jnp.where(iota(value.shape, 1) < CENTER, value, 0.0)
                classed[c * wide : (c + 1) * wide, k * LANES : (k + 1) * LANES] = value.astype(
                    jnp.bfloat16
                )
        weights = jnp.concatenate(
            [
                lane_pick(
                    taps[0][v * slab + s : v * slab + s + 1],
                    jnp.clip(base_x - shift(v, s, 0), 0, LANES - 1),
                ).astype(jnp.bfloat16)
                for v in range(VIEWS)
            ],
            axis=1,
        )
        for k in range(blocks):
            part = jnp.dot(
                classed[:, k * LANES : (k + 2) * LANES],
                weights,
                preferred_element_type=jnp.float32,
            ).astype(jnp.bfloat16)
            for v in range(VIEWS):
                moved[v, :, k * LANES : (k + 1) * LANES] = part[:, v * LANES : (v + 1) * LANES]
        for v in range(VIEWS):
            index = jnp.clip(base_y - shift(v, s, 1), 0, LANES - 1)
            row = taps[1][v * slab + s : v * slab + s + 1]
            weights = jnp.concatenate(
                [
                    lane_pick(row, index[:, j * LANES : (j + 1) * LANES]).astype(jnp.bfloat16)
                    for j in range(4 * wide // LANES)
                ],
                axis=1,
            )
            facing = view[v, 3] >= 0
            for k in range(0, width, 256):
                sheared = jnp.dot(
                    weights, moved[v, :, k : k + 256], preferred_element_type=jnp.float32
                )
                if s == 0:
                    picture[v, :, k : k + 256] = sheared
                    continue
                before = picture[v, :, k : k + 256]
                front = jnp.where(facing, before, sheared)
                back = jnp.where(facing, sheared, before)
                through = 1.0 - front[3 * rows :]
                picture[v, :, k : k + 256] = front + jnp.concatenate([through] * 4, axis=0) * back
    strips = out.shape[0]
    strip = width // strips
    for v in range(VIEWS):
        for k in range(blocks):
            turned = picture[v, :, k * LANES : (k + 1) * LANES].T.astype(jnp.bfloat16)
            per = LANES // strip
            out[k * per : (k + 1) * per, v * strip : (v + 1) * strip, :] = turned.reshape(
                per, strip, 4 * rows
            )


def gather_kernel(ids, view, arrived, strip_out, send_a, send_b):
    slabs, both, lanes = arrived.shape
    strip = both // VIEWS
    rows = lanes // 4
    pick = 3 * rows + iota((strip, lanes), 1) % rows
    even = ids[0] % 2 == 0
    for v in range(VIEWS):
        facing = view[v, 3] >= 0
        picture = jnp.zeros((strip, lanes), jnp.float32)
        through = jnp.ones((strip, lanes), jnp.float32)
        for k in range(slabs):
            at = jnp.where(facing, k, slabs - 1 - k)
            part = arrived[at, v * strip : (v + 1) * strip, :].astype(jnp.float32)
            picture = picture + through * part
            through = through * (
                1.0 - jnp.take_along_axis(part, pick, axis=1, mode="promise_in_bounds")
            )
        strip_out[v] = picture
        first = picture[:HALO]
        last = picture[strip - HALO :]
        send_a[v] = jnp.where(even, last, first)
        send_b[v] = jnp.where(even, first, last)


def warp_kernel(ids, view, strip_in, got_a, got_b, out):
    strip, lanes = strip_in.shape[1:]
    width = strip * ids[2]
    even = ids[0] % 2 == 0
    shape = (strip, strip + 2 * HALO)
    start_a = jnp.where(even, strip, -HALO)
    start_b = jnp.where(even, -HALO, strip)
    at = iota(shape, 1)
    local = jnp.where(
        at < strip,
        at,
        jnp.where(at < strip + HALO, at - strip + start_a, at - strip - HALO + start_b),
    )
    column = iota(shape, 0)
    for v in range(VIEWS):
        num = view[v, 2] * (2 * (ids[0] * strip + column) + 1 - width) + width
        whole = num // (2 * width)
        frac = (num - whole * (2 * width)).astype(jnp.float32) / (2.0 * width.astype(jnp.float32))
        weights = lanczos(frac - (local - column - whole).astype(jnp.float32))
        source = jnp.concatenate([strip_in[v], got_a[v], got_b[v]], axis=0)
        out[v] = jnp.dot(
            weights,
            source,
            precision=lax.Precision.HIGHEST,
            preferred_element_type=jnp.float32,
        )


def call(kernel, outs, scratch=(), vmem_from=2):
    def run(*args):
        return pl.pallas_call(
            kernel,
            out_shape=outs,
            in_specs=[pl.BlockSpec(memory_space=pltpu.SMEM)] * vmem_from
            + [pl.BlockSpec(memory_space=pltpu.VMEM)] * (len(args) - vmem_from),
            out_specs=jax.tree.map(lambda _: pl.BlockSpec(memory_space=pltpu.VMEM), outs),
            scratch_shapes=list(scratch),
            compiler_params=pltpu.CompilerParams(vmem_limit_bytes=VMEM_LIMIT),
        )(*args)

    return run


def body(volume, tf_table, view_code):
    slab, rows, width = volume.shape
    depth_size = lax.axis_size("depth")
    band_size = lax.axis_size("band")
    depth_rank = lax.axis_index("depth")
    band_rank = lax.axis_index("band")
    strip = width // depth_size
    wide = rows + 2 * HALO
    lanes = 4 * rows
    ids = jnp.stack(
        [depth_rank, band_rank, jnp.int32(depth_size), jnp.int32(band_size)]
    ).astype(jnp.int32)
    even = band_rank % 2 == 0
    first = volume[:, :HALO]
    last = volume[:, rows - HALO :]
    got_a = lax.ppermute(
        jnp.where(even, last, first).astype(jnp.bfloat16), "band", pairs(band_size, 0)
    )
    got_b = lax.ppermute(
        jnp.where(even, first, last).astype(jnp.bfloat16), "band", pairs(band_size, 1)
    )
    pieces = call(
        shear_kernel,
        jax.ShapeDtypeStruct((depth_size, VIEWS * strip, lanes), jnp.bfloat16),
        (
            pltpu.VMEM((4 * wide, width + LANES), jnp.bfloat16),
            pltpu.VMEM((VIEWS, 4 * wide, width), jnp.bfloat16),
            pltpu.VMEM((VIEWS, lanes, width), jnp.float32),
        ),
    )(ids, view_code, tf_table, volume, got_a, got_b)
    arrived = lax.all_to_all(pieces, "depth", split_axis=0, concat_axis=0, tiled=True)
    edge = jax.ShapeDtypeStruct((VIEWS, HALO, lanes), jnp.float32)
    whole = jax.ShapeDtypeStruct((VIEWS, strip, lanes), jnp.float32)
    middle, send_a, send_b = call(gather_kernel, (whole, edge, edge))(ids, view_code, arrived)
    side_a = lax.ppermute(send_a, "depth", pairs(depth_size, 0))
    side_b = lax.ppermute(send_b, "depth", pairs(depth_size, 1))
    final = call(warp_kernel, whole)(ids, view_code, middle, side_a, side_b)
    return final.reshape(VIEWS, strip, 4, rows)


def solution(mesh):
    placed = (P("depth", "band", None), P(), P())
    return jax.shard_map(
        body, mesh=mesh, in_specs=placed, out_specs=P(None, "depth", None, "band"), check_vma=False
    )
```

```python
import jax
import jax.numpy as jnp
from jax import lax
from jax.experimental import pallas as pl
from jax.experimental.pallas import tpu as pltpu
from jax.sharding import PartitionSpec as P

VIEWS = 2
HALO = 16
LANES = 128
CENTER = 64
VMEM_LIMIT = 16 * 2**20


def sinc(t):
    angle = jnp.where(t == 0.0, 1.0, jnp.pi * t)
    return jnp.where(t == 0.0, 1.0, jnp.sin(angle) / angle)


def lanczos(offset):
    return jnp.where(jnp.abs(offset) < 3.0, sinc(offset) * sinc(offset / 3.0), 0.0)


def iota(shape, dim):
    return lax.broadcasted_iota(jnp.int32, shape, dim)


def pairs(size, first):
    out = []
    for a in range(first, size - 1, 2):
        out += [(a, a + 1), (a + 1, a)]
    return out


def lane_pick(row, index):
    table = jnp.broadcast_to(row, index.shape)
    return jnp.take_along_axis(table, index, axis=1, mode="promise_in_bounds")


def classify(code, palette, out, k, last, group):
    high = code >= LANES
    low = code & (LANES - 1)
    for c in range(4):
        value = jnp.where(
            high,
            lane_pick(palette[c : c + 1, LANES:], low),
            lane_pick(palette[c : c + 1, :LANES], low),
        )
        if k == 0:
            value = jnp.where(iota(value.shape, 1) >= CENTER, value, 0.0)
        if k == last:
            value = jnp.where(iota(value.shape, 1) < CENTER, value, 0.0)
        out[c * group : (c + 1) * group, k * LANES : (k + 1) * LANES] = value.astype(jnp.bfloat16)


def shear_columns(voxels, palette, weights, classed, store):
    group, width = voxels.shape
    blocks = width // LANES
    side = jnp.zeros((group, CENTER), jnp.int32)
    voxels = jnp.concatenate([side, voxels, side], axis=1)
    for k in range(blocks + 1):
        classify(voxels[:, k * LANES : (k + 1) * LANES], palette, classed, k, blocks, group)
    for k in range(blocks):
        part = jnp.dot(
            classed[:, k * LANES : (k + 2) * LANES], weights, preferred_element_type=jnp.float32
        ).astype(jnp.bfloat16)
        for v in range(VIEWS):
            store(v, k, part[:, v * LANES : (v + 1) * LANES])


def own_kernel(ids, view, tf, vol, own, filter_x, filter_y, filter_w, palette_out, classed):
    slab, rows, width = vol.shape
    depth_rank, band_rank = ids[0], ids[1]
    depth = slab * ids[2]
    height = rows * ids[3]
    strip = filter_w.shape[1]

    codes = tf[...].astype(jnp.float32)
    opacity = codes[3:4] / (64.0 * depth.astype(jnp.float32))
    premult = codes[0:3] / 255.0 * opacity
    palette = jnp.concatenate([premult, opacity], axis=0).astype(jnp.bfloat16).astype(jnp.float32)
    palette_out[...] = palette

    which = iota((VIEWS * slab, LANES), 0)
    lane = iota((VIEWS * slab, LANES), 1)
    place = depth_rank * slab + which % slab
    taps = []
    for column in range(2):
        q = jnp.where(which < slab, view[0, column], view[1, column])
        num = q * (2 * place + 1 - depth)
        whole = num // (2 * depth)
        frac = (num - whole * (2 * depth)).astype(jnp.float32) / (2.0 * depth.astype(jnp.float32))
        taps.append(
            lanczos(frac - (lane - CENTER).astype(jnp.float32))
            .astype(jnp.bfloat16)
            .astype(jnp.float32)
        )

    def shift(v, s, column):
        num = view[v, column] * (2 * (depth_rank * slab + s) + 1 - depth)
        return num // (2 * depth)

    base_x = iota((2 * LANES, LANES), 0) - iota((2 * LANES, LANES), 1)
    for s in range(slab):
        for v in range(VIEWS):
            row = taps[0][v * slab + s : v * slab + s + 1]
            index = jnp.clip(base_x - shift(v, s, 0), 0, LANES - 1)
            filter_x[s, :, v * LANES : (v + 1) * LANES] = lane_pick(row, index).astype(jnp.bfloat16)

        def store(v, k, part):
            own[v, s, :, k * LANES : (k + 1) * LANES] = part

        shear_columns(vol[s], palette, filter_x[s], classed, store)

    lanes = 4 * rows
    to = iota((lanes, lanes), 0)
    frm = iota((lanes, lanes), 1)
    even = band_rank % 2 == 0
    start_a = jnp.where(even, rows, -HALO)
    start_b = jnp.where(even, -HALO, rows)
    at = frm % rows
    base_y = []
    for local in (at, jnp.where(at < HALO, at + start_a, at - HALO + start_b)):
        world = local + band_rank * rows
        fits = (to // rows == frm // rows) & (world >= 0) & (world < height)
        base_y.append(jnp.where(fits, local - to % rows + CENTER, -4 * LANES))
    for v in range(VIEWS):
        for s in range(slab):
            row = taps[1][v * slab + s : v * slab + s + 1]
            for j in range(2):
                index = jnp.clip(base_y[j] - shift(v, s, 1), 0, LANES - 1)
                filter_y[v, s, :, j * lanes : (j + 1) * lanes] = lane_pick(row, index).astype(
                    jnp.bfloat16
                )

    even = depth_rank % 2 == 0
    shape = (strip, strip + 2 * HALO)
    start_a = jnp.where(even, strip, -HALO)
    start_b = jnp.where(even, -HALO, strip)
    at = iota(shape, 1)
    local = jnp.where(
        at < strip,
        at,
        jnp.where(at < strip + HALO, at - strip + start_a, at - strip - HALO + start_b),
    )
    column = iota(shape, 0)
    for v in range(VIEWS):
        num = view[v, 2] * (2 * (depth_rank * strip + column) + 1 - width) + width
        whole = num // (2 * width)
        frac = (num - whole * (2 * width)).astype(jnp.float32) / (2.0 * width)
        filter_w[v] = lanczos(frac - (local - column - whole).astype(jnp.float32))


def slab_kernel(
    ids, view, palette, filter_x, filter_y, own, got_a, got_b, keep, send, classed, near
):
    slab = own.shape[1]
    lanes, width = own.shape[2:]
    rows = lanes // 4
    strip = keep.shape[1] // VIEWS
    for s in range(slab):

        def store(v, k, part):
            near[v, s, :, k * LANES : (k + 1) * LANES] = part

        voxels = jnp.concatenate(
            [got_a[s].astype(jnp.int32), got_b[s].astype(jnp.int32)], axis=0
        )
        shear_columns(voxels, palette[...], filter_x[s], classed, store)
    chunk = 2 * LANES
    per = chunk // (2 * strip)
    first = ids[0] % 2 == 0
    for v in range(VIEWS):
        facing = view[v, 3] >= 0
        for k in range(width // chunk):
            for step in range(slab):
                s = jnp.where(facing, step, slab - 1 - step)
                source = jnp.concatenate(
                    [
                        own[v, s, :, k * chunk : (k + 1) * chunk],
                        near[v, s, :, k * chunk : (k + 1) * chunk],
                    ],
                    axis=0,
                )
                sheared = jnp.dot(filter_y[v, s], source, preferred_element_type=jnp.float32)
                if step == 0:
                    picture = sheared
                    continue
                through = 1.0 - picture[3 * rows :]
                picture = picture + jnp.concatenate([through] * 4, axis=0) * sheared
            turned = picture.T.reshape(per, 2, strip, lanes)
            even, odd = turned[:, 0], turned[:, 1]
            at = slice(k * per, (k + 1) * per)
            keep[at, v * strip : (v + 1) * strip] = jnp.where(first, even, odd)
            send[at, v * strip : (v + 1) * strip] = jnp.where(first, odd, even).astype(
                jnp.bfloat16
            )


def merge_kernel(ids, view, keep, got, out):
    strips, both, lanes = keep.shape
    strip = both // VIEWS
    rows = lanes // 4
    first = ids[0] % 2 == 0
    pick = 3 * rows + iota((strip, lanes), 1) % rows
    for v in range(VIEWS):
        mine_front = (view[v, 3] >= 0) == first
        for k in range(strips):
            mine = keep[k, v * strip : (v + 1) * strip]
            other = got[k, v * strip : (v + 1) * strip].astype(jnp.float32)
            front = jnp.where(mine_front, mine, other)
            back = jnp.where(mine_front, other, mine)
            alpha = jnp.take_along_axis(front, pick, axis=1, mode="promise_in_bounds")
            out[k, v * strip : (v + 1) * strip] = (front + (1.0 - alpha) * back).astype(
                jnp.bfloat16
            )


def gather_kernel(ids, view, arrived, strip_out, send_a, send_b):
    slabs, both, lanes = arrived.shape
    strip = both // VIEWS
    rows = lanes // 4
    pick = 3 * rows + iota((strip, lanes), 1) % rows
    even = ids[0] % 2 == 0
    for v in range(VIEWS):
        facing = view[v, 3] >= 0
        picture = jnp.zeros((strip, lanes), jnp.float32)
        through = jnp.ones((strip, lanes), jnp.float32)
        for k in range(slabs):
            at = jnp.where(facing, k, slabs - 1 - k)
            part = arrived[at, v * strip : (v + 1) * strip, :].astype(jnp.float32)
            picture = picture + through * part
            through = through * (
                1.0 - jnp.take_along_axis(part, pick, axis=1, mode="promise_in_bounds")
            )
        strip_out[v] = picture
        first = picture[:HALO]
        last = picture[strip - HALO :]
        send_a[v] = jnp.where(even, last, first)
        send_b[v] = jnp.where(even, first, last)


def warp_kernel(filter_w, strip_in, got_a, got_b, out):
    rows = strip_in.shape[2] // 4
    for v in range(VIEWS):
        source = jnp.concatenate([strip_in[v], got_a[v], got_b[v]], axis=0)
        final = jnp.dot(
            filter_w[v],
            source,
            precision=lax.Precision.HIGHEST,
            preferred_element_type=jnp.float32,
        )
        for c in range(4):
            out[v, :, c, :] = final[:, c * rows : (c + 1) * rows]


def call(kernel, outs, scratch=(), vmem_from=2):
    def run(*args):
        return pl.pallas_call(
            kernel,
            out_shape=outs,
            in_specs=[pl.BlockSpec(memory_space=pltpu.SMEM)] * vmem_from
            + [pl.BlockSpec(memory_space=pltpu.VMEM)] * (len(args) - vmem_from),
            out_specs=jax.tree.map(lambda _: pl.BlockSpec(memory_space=pltpu.VMEM), outs),
            scratch_shapes=list(scratch),
            compiler_params=pltpu.CompilerParams(vmem_limit_bytes=VMEM_LIMIT),
        )(*args)

    return run


def body(volume, tf_table, view_code):
    slab, rows, width = volume.shape
    depth_size = lax.axis_size("depth")
    band_size = lax.axis_size("band")
    depth_rank = lax.axis_index("depth")
    band_rank = lax.axis_index("band")
    strip = width // depth_size
    lanes = 4 * rows
    bf16, f32 = jnp.bfloat16, jnp.float32
    ids = jnp.stack(
        [depth_rank, band_rank, jnp.int32(depth_size), jnp.int32(band_size)]
    ).astype(jnp.int32)
    even = band_rank % 2 == 0
    first = volume[:, :HALO]
    last = volume[:, rows - HALO :]
    got_a = lax.ppermute(jnp.where(even, last, first).astype(bf16), "band", pairs(band_size, 0))
    got_b = lax.ppermute(jnp.where(even, first, last).astype(bf16), "band", pairs(band_size, 1))
    own, filter_x, filter_y, filter_w, palette = call(
        own_kernel,
        (
            jax.ShapeDtypeStruct((VIEWS, slab, lanes, width), bf16),
            jax.ShapeDtypeStruct((slab, 2 * LANES, VIEWS * LANES), bf16),
            jax.ShapeDtypeStruct((VIEWS, slab, lanes, 2 * lanes), bf16),
            jax.ShapeDtypeStruct((VIEWS, strip, strip + 2 * HALO), f32),
            jax.ShapeDtypeStruct(tf_table.shape, f32),
        ),
        (pltpu.VMEM((lanes, width + LANES), bf16),),
    )(ids, view_code, tf_table, volume)
    half = (depth_size // 2, VIEWS * strip, lanes)
    keep, send = call(
        slab_kernel,
        (jax.ShapeDtypeStruct(half, f32), jax.ShapeDtypeStruct(half, bf16)),
        (
            pltpu.VMEM((8 * HALO, width + LANES), bf16),
            pltpu.VMEM((VIEWS, slab, 8 * HALO, width), bf16),
        ),
    )(ids, view_code, palette, filter_x, filter_y, own, got_a, got_b)
    got = lax.ppermute(send, "depth", pairs(depth_size, 0))
    merged = call(merge_kernel, jax.ShapeDtypeStruct(half, bf16))(ids, view_code, keep, got)
    arrived = lax.all_to_all(
        merged,
        "depth",
        split_axis=0,
        concat_axis=0,
        tiled=True,
        axis_index_groups=[list(range(i, depth_size, 2)) for i in range(2)],
    )
    edge = jax.ShapeDtypeStruct((VIEWS, HALO, lanes), f32)
    whole = jax.ShapeDtypeStruct((VIEWS, strip, lanes), f32)
    middle, send_a, send_b = call(gather_kernel, (whole, edge, edge))(ids, view_code, arrived)
    side_a = lax.ppermute(send_a, "depth", pairs(depth_size, 0))
    side_b = lax.ppermute(send_b, "depth", pairs(depth_size, 1))
    final = jax.ShapeDtypeStruct((VIEWS, strip, 4, rows), f32)
    return call(warp_kernel, final, (), 0)(filter_w, middle, side_a, side_b)


def solution(mesh):
    placed = (P("depth", "band", None), P(), P())
    return jax.shard_map(
        body, mesh=mesh, in_specs=placed, out_specs=P(None, "depth", None, "band"), check_vma=False
    )
```

```python
import jax
import jax.numpy as jnp
from jax import lax
from jax.experimental import pallas as pl
from jax.experimental.pallas import tpu as pltpu
from jax.sharding import PartitionSpec as P

VIEWS = 2
HALO = 16
LANES = 128
CENTER = 64
VMEM_LIMIT = 16 * 2**20


def sinc(t):
    angle = jnp.where(t == 0.0, 1.0, jnp.pi * t)
    return jnp.where(t == 0.0, 1.0, jnp.sin(angle) / angle)


def lanczos(offset):
    return jnp.where(jnp.abs(offset) < 3.0, sinc(offset) * sinc(offset / 3.0), 0.0)


def iota(shape, dim):
    return lax.broadcasted_iota(jnp.int32, shape, dim)


def pairs(size, first):
    out = []
    for a in range(first, size - 1, 2):
        out += [(a, a + 1), (a + 1, a)]
    return out


def lane_pick(row, index):
    table = jnp.broadcast_to(row, index.shape)
    return jnp.take_along_axis(table, index, axis=1, mode="promise_in_bounds")


def classify(code, palette, out, k, last, group):
    high = code >= LANES
    low = code & (LANES - 1)
    for c in range(4):
        value = jnp.where(
            high,
            lane_pick(palette[c : c + 1, LANES:], low),
            lane_pick(palette[c : c + 1, :LANES], low),
        )
        if k == 0:
            value = jnp.where(iota(value.shape, 1) >= CENTER, value, 0.0)
        if k == last:
            value = jnp.where(iota(value.shape, 1) < CENTER, value, 0.0)
        out[c * group : (c + 1) * group, k * LANES : (k + 1) * LANES] = value.astype(jnp.bfloat16)


def shear_columns(voxels, palette, weights, classed, store):
    group, width = voxels.shape
    blocks = width // LANES
    side = jnp.zeros((group, CENTER), jnp.int32)
    voxels = jnp.concatenate([side, voxels, side], axis=1)
    for k in range(blocks + 1):
        classify(voxels[:, k * LANES : (k + 1) * LANES], palette, classed, k, blocks, group)
    for k in range(blocks):
        part = jnp.dot(
            classed[:, k * LANES : (k + 2) * LANES], weights, preferred_element_type=jnp.float32
        ).astype(jnp.bfloat16)
        for v in range(VIEWS):
            store(v, k, part[:, v * LANES : (v + 1) * LANES])


def own_kernel(
    scalars, tables, vol, params, palette_out, own, filter_x, filter_y, filter_w, classed
):
    slab, rows, width = vol.shape
    for i in range(1 + VIEWS):
        for j in range(4):
            params[i, j] = scalars[4 + i, j]
    depth_rank, band_rank = scalars[4, 0], scalars[4, 1]
    depth = slab * scalars[4, 2]
    height = rows * scalars[4, 3]
    strip = filter_w.shape[1]

    codes = tables[0:4].astype(jnp.float32)
    opacity = codes[3:4] / (64.0 * depth.astype(jnp.float32))
    premult = codes[0:3] / 255.0 * opacity
    palette = jnp.concatenate([premult, opacity], axis=0).astype(jnp.bfloat16).astype(jnp.float32)
    palette_out[...] = palette

    which = iota((VIEWS * slab, LANES), 0)
    lane = iota((VIEWS * slab, LANES), 1)
    place = depth_rank * slab + which % slab
    taps = []
    for column in range(2):
        q = jnp.where(which < slab, scalars[5, column], scalars[6, column])
        num = q * (2 * place + 1 - depth)
        whole = num // (2 * depth)
        frac = (num - whole * (2 * depth)).astype(jnp.float32) / (2.0 * depth.astype(jnp.float32))
        taps.append(
            lanczos(frac - (lane - CENTER).astype(jnp.float32))
            .astype(jnp.bfloat16)
            .astype(jnp.float32)
        )

    def shift(v, s, column):
        num = scalars[5 + v, column] * (2 * (depth_rank * slab + s) + 1 - depth)
        return num // (2 * depth)

    base_x = iota((2 * LANES, LANES), 0) - iota((2 * LANES, LANES), 1)
    for s in range(slab):
        for v in range(VIEWS):
            row = taps[0][v * slab + s : v * slab + s + 1]
            index = jnp.clip(base_x - shift(v, s, 0), 0, LANES - 1)
            filter_x[s, :, v * LANES : (v + 1) * LANES] = lane_pick(row, index).astype(jnp.bfloat16)

        def store(v, k, part):
            own[v, s, :, k * LANES : (k + 1) * LANES] = part

        shear_columns(vol[s].astype(jnp.int32), palette, filter_x[s], classed, store)

    lanes = 4 * rows
    to = iota((lanes, lanes), 0)
    frm = iota((lanes, lanes), 1)
    even = band_rank % 2 == 0
    start_a = jnp.where(even, rows, -HALO)
    start_b = jnp.where(even, -HALO, rows)
    at = frm % rows
    base_y = []
    for local in (at, jnp.where(at < HALO, at + start_a, at - HALO + start_b)):
        world = local + band_rank * rows
        fits = (to // rows == frm // rows) & (world >= 0) & (world < height)
        base_y.append(jnp.where(fits, local - to % rows + CENTER, -4 * LANES))
    for v in range(VIEWS):
        for s in range(slab):
            row = taps[1][v * slab + s : v * slab + s + 1]
            for j in range(2):
                index = jnp.clip(base_y[j] - shift(v, s, 1), 0, LANES - 1)
                filter_y[v, s, :, j * lanes : (j + 1) * lanes] = lane_pick(row, index).astype(
                    jnp.bfloat16
                )

    shape = (strip, strip + 2 * HALO)
    local = iota(shape, 1) - HALO
    column = iota(shape, 0)
    for v in range(VIEWS):
        num = scalars[5 + v, 2] * (2 * (depth_rank * strip + column) + 1 - width) + width
        whole = num // (2 * width)
        frac = (num - whole * (2 * width)).astype(jnp.float32) / (2.0 * width)
        filter_w[v] = lanczos(frac - (local - column - whole).astype(jnp.float32))


def slab_kernel(
    params, palette, filter_x, filter_y, own, got_a, got_b, keep, send, classed, near
):
    slab = own.shape[1]
    lanes, width = own.shape[2:]
    rows = lanes // 4
    for s in range(slab):

        def store(v, k, part):
            near[v, s, :, k * LANES : (k + 1) * LANES] = part

        voxels = jnp.concatenate(
            [got_a[s].astype(jnp.int32), got_b[s].astype(jnp.int32)], axis=0
        )
        shear_columns(voxels, palette[...], filter_x[s], classed, store)
    chunk = 2 * LANES
    for v in range(VIEWS):
        facing = params[1 + v, 3] >= 0
        for side in (slice(0, HALO), slice(HALO + width, 2 * HALO + width)):
            keep[v, side] = jnp.zeros((HALO, lanes), jnp.float32)
            send[v, side] = jnp.zeros((HALO, lanes), jnp.bfloat16)
        for k in range(width // chunk):
            for step in range(slab):
                s = jnp.where(facing, step, slab - 1 - step)
                source = jnp.concatenate(
                    [
                        own[v, s, :, k * chunk : (k + 1) * chunk],
                        near[v, s, :, k * chunk : (k + 1) * chunk],
                    ],
                    axis=0,
                )
                sheared = jnp.dot(filter_y[v, s], source, preferred_element_type=jnp.float32)
                if step == 0:
                    picture = sheared
                    continue
                through = 1.0 - picture[3 * rows :]
                picture = picture + jnp.concatenate([through] * 4, axis=0) * sheared
            turned = picture.T
            at = slice(HALO + k * chunk, HALO + (k + 1) * chunk)
            keep[v, at] = turned
            send[v, at] = turned.astype(jnp.bfloat16)


def merge_kernel(params, keep, got, out):
    strips, both, lanes = out.shape
    span = both // VIEWS
    rows = lanes // 4
    core = params[0, 0] % 2
    pick = 3 * rows + iota((span, lanes), 1) % rows
    for v in range(VIEWS):
        mine_front = (params[1 + v, 3] >= 0) == (core == 0)
        for k in range(strips):
            at = pl.ds(pl.multiple_of(k * span + core * (span // 2), span // 2), span)
            mine = keep[v, at]
            other = got[v, at].astype(jnp.float32)
            front = jnp.where(mine_front, mine, other)
            back = jnp.where(mine_front, other, mine)
            alpha = jnp.take_along_axis(front, pick, axis=1, mode="promise_in_bounds")
            out[k, v * span : (v + 1) * span] = (front + (1.0 - alpha) * back).astype(
                jnp.bfloat16
            )


def final_kernel(params, filter_w, arrived, out):
    slabs, both, lanes = arrived.shape
    span = both // VIEWS
    rows = lanes // 4
    pick = 3 * rows + iota((span, lanes), 1) % rows
    for v in range(VIEWS):
        facing = params[1 + v, 3] >= 0
        picture = jnp.zeros((span, lanes), jnp.float32)
        through = jnp.ones((span, lanes), jnp.float32)
        for k in range(slabs):
            at = jnp.where(facing, k, slabs - 1 - k)
            part = arrived[at, v * span : (v + 1) * span, :].astype(jnp.float32)
            picture = picture + through * part
            through = through * (
                1.0 - jnp.take_along_axis(part, pick, axis=1, mode="promise_in_bounds")
            )
        final = jnp.dot(
            filter_w[v],
            picture,
            precision=lax.Precision.HIGHEST,
            preferred_element_type=jnp.float32,
        )
        for c in range(4):
            out[v, :, c, :] = final[:, c * rows : (c + 1) * rows]


def call(kernel, outs, scratch=(), spaces=(), out_spaces=None):
    def run(*args):
        given = list(spaces) + [pltpu.VMEM] * (len(args) - len(spaces))
        where = out_spaces or jax.tree.map(lambda _: pltpu.VMEM, outs)
        return pl.pallas_call(
            kernel,
            out_shape=outs,
            in_specs=[pl.BlockSpec(memory_space=space) for space in given],
            out_specs=jax.tree.map(lambda space: pl.BlockSpec(memory_space=space), where),
            scratch_shapes=list(scratch),
            compiler_params=pltpu.CompilerParams(vmem_limit_bytes=VMEM_LIMIT),
        )(*args)

    return run


def body(volume, tf_table, view_code):
    slab, rows, width = volume.shape
    depth_size = lax.axis_size("depth")
    band_size = lax.axis_size("band")
    strip = width // depth_size
    lanes = 4 * rows
    bf16, f32, i32 = jnp.bfloat16, jnp.float32, jnp.int32
    shape = jax.ShapeDtypeStruct
    smem = (pltpu.SMEM,)
    ids = jnp.stack(
        [lax.axis_index("depth"), lax.axis_index("band"), jnp.int32(depth_size), jnp.int32(band_size)]
    ).astype(i32)
    wide = tf_table.shape[1]
    tables = jnp.concatenate(
        [tf_table]
        + [jnp.pad(part, ((0, 0), (0, wide - 4))) for part in (ids[None], view_code)]
        + [jnp.zeros((1, wide), i32)],
        axis=0,
    )
    voxels = volume.astype(bf16)
    even = lax.axis_index("band") % 2 == 0
    first = voxels[:, :HALO]
    last = voxels[:, rows - HALO :]
    send_a = jnp.where(even, last, first)
    send_b = jnp.where(even, first, last)
    got_a = lax.ppermute(send_a, "band", pairs(band_size, 0))
    got_b = lax.ppermute(send_b, "band", pairs(band_size, 1))
    params, palette, own, filter_x, filter_y, filter_w = call(
        own_kernel,
        (
            shape((1 + VIEWS, 4), i32),
            shape(tf_table.shape, f32),
            shape((VIEWS, slab, lanes, width), bf16),
            shape((slab, 2 * LANES, VIEWS * LANES), bf16),
            shape((VIEWS, slab, lanes, 2 * lanes), bf16),
            shape((VIEWS, strip, strip + 2 * HALO), f32),
        ),
        (pltpu.VMEM((lanes, width + LANES), bf16),),
        smem,
        (pltpu.SMEM,) + (pltpu.VMEM,) * 5,
    )(tables, tables, voxels)
    padded = (VIEWS, width + 2 * HALO, lanes)
    keep, send = call(
        slab_kernel,
        (shape(padded, f32), shape(padded, bf16)),
        (
            pltpu.VMEM((8 * HALO, width + LANES), bf16),
            pltpu.VMEM((VIEWS, slab, 8 * HALO, width), bf16),
        ),
        smem,
    )(params, palette, filter_x, filter_y, own, got_a, got_b)
    got = lax.ppermute(send, "depth", pairs(depth_size, 0))
    merged = shape((depth_size // 2, VIEWS * (strip + 2 * HALO), lanes), bf16)
    merged = call(merge_kernel, merged, (), smem)(params, keep, got)
    arrived = lax.all_to_all(
        merged,
        "depth",
        split_axis=0,
        concat_axis=0,
        tiled=True,
        axis_index_groups=[list(range(i, depth_size, 2)) for i in range(2)],
    )
    final = shape((VIEWS, strip, 4, rows), f32)
    return call(final_kernel, final, (), smem)(params, filter_w, arrived)


def solution(mesh):
    placed = (P("depth", "band", None), P(), P())
    return jax.shard_map(
        body, mesh=mesh, in_specs=placed, out_specs=P(None, "depth", None, "band"), check_vma=False
    )
```

```python
import jax
import jax.numpy as jnp
from jax import lax
from jax.experimental import pallas as pl
from jax.experimental.pallas import tpu as pltpu
from jax.sharding import PartitionSpec as P

VIEWS = 2
HALO = 16
MARGIN = 12
LANES = 128
CENTER = 64
FAR = 20
VMEM_LIMIT = 16 * 2**20


def sinc(t):
    angle = jnp.where(t == 0.0, 1.0, jnp.pi * t)
    return jnp.where(t == 0.0, 1.0, jnp.sin(angle) / angle)


def lanczos(offset):
    return jnp.where(jnp.abs(offset) < 3.0, sinc(offset) * sinc(offset / 3.0), 0.0)


def iota(shape, dim):
    return lax.broadcasted_iota(jnp.int32, shape, dim)


def pairs(size, first):
    out = []
    for a in range(first, size - 1, 2):
        out += [(a, a + 1), (a + 1, a)]
    return out


def lane_pick(row, index):
    table = jnp.broadcast_to(row, index.shape)
    return jnp.take_along_axis(table, index, axis=1, mode="promise_in_bounds")


def classify(code, palette, out, k, last, group):
    high = code >= LANES
    low = code & (LANES - 1)
    for c in range(4):
        value = jnp.where(
            high,
            lane_pick(palette[c : c + 1, LANES:], low),
            lane_pick(palette[c : c + 1, :LANES], low),
        )
        if k == 0:
            value = jnp.where(iota(value.shape, 1) >= CENTER, value, 0.0)
        if k == last:
            value = jnp.where(iota(value.shape, 1) < CENTER, value, 0.0)
        out[c * group : (c + 1) * group, k * LANES : (k + 1) * LANES] = value.astype(jnp.bfloat16)


def shear_columns(voxels, palette, weights, classed, store):
    group, width = voxels.shape
    blocks = width // LANES
    side = jnp.zeros((group, CENTER), jnp.int32)
    voxels = jnp.concatenate([side, voxels, side], axis=1)
    for k in range(blocks + 1):
        classify(voxels[:, k * LANES : (k + 1) * LANES], palette, classed, k, blocks, group)
    for k in range(blocks):
        part = jnp.dot(
            classed[:, k * LANES : (k + 2) * LANES], weights, preferred_element_type=jnp.float32
        ).astype(jnp.bfloat16)
        for v in range(VIEWS):
            store(v, k, part[:, v * LANES : (v + 1) * LANES])


def own_kernel(
    scalars, tables, vol, params, palette_out, own, filter_x, filter_y, filter_w, classed
):
    slab, rows, width = vol.shape
    for i in range(1 + VIEWS):
        for j in range(4):
            params[i, j] = scalars[4 + i, j]
    depth_rank, band_rank = scalars[4, 0], scalars[4, 1]
    depth = slab * scalars[4, 2]
    height = rows * scalars[4, 3]
    strip = filter_w.shape[0]

    codes = tables[0:4].astype(jnp.float32)
    opacity = codes[3:4] / (64.0 * depth.astype(jnp.float32))
    premult = codes[0:3] / 255.0 * opacity
    palette = jnp.concatenate([premult, opacity], axis=0).astype(jnp.bfloat16).astype(jnp.float32)
    palette_out[...] = palette

    which = iota((VIEWS * slab, LANES), 0)
    lane = iota((VIEWS * slab, LANES), 1)
    place = depth_rank * slab + which % slab
    taps = []
    for column in range(2):
        q = jnp.where(which < slab, scalars[5, column], scalars[6, column])
        num = q * (2 * place + 1 - depth)
        whole = num // (2 * depth)
        frac = (num - whole * (2 * depth)).astype(jnp.float32) / (2.0 * depth.astype(jnp.float32))
        taps.append(
            lanczos(frac - (lane - CENTER).astype(jnp.float32))
            .astype(jnp.bfloat16)
            .astype(jnp.float32)
        )

    def shift(v, s, column):
        num = scalars[5 + v, column] * (2 * (depth_rank * slab + s) + 1 - depth)
        return num // (2 * depth)

    base_x = iota((2 * LANES, LANES), 0) - iota((2 * LANES, LANES), 1)
    base_x = jnp.clip(base_x, FAR, LANES - 1 - FAR)
    for s in range(slab):
        for v in range(VIEWS):
            row = taps[0][v * slab + s : v * slab + s + 1]
            index = base_x - shift(v, s, 0)
            filter_x[s, :, v * LANES : (v + 1) * LANES] = lane_pick(row, index).astype(jnp.bfloat16)

        def store(v, k, part):
            own[v, s, :, k * LANES : (k + 1) * LANES] = part

        shear_columns(vol[s].astype(jnp.int32), palette, filter_x[s], classed, store)

    lanes = 4 * rows
    to = iota((lanes, lanes), 0)
    frm = iota((lanes, lanes), 1)
    even = band_rank % 2 == 0
    start_a = jnp.where(even, rows, -HALO)
    start_b = jnp.where(even, -HALO, rows)
    at = frm % rows
    base_y = []
    for local in (at, jnp.where(at < HALO, at + start_a, at - HALO + start_b)):
        world = local + band_rank * rows
        fits = (to // rows == frm // rows) & (world >= 0) & (world < height)
        base_y.append(jnp.where(fits, local - to % rows + CENTER, FAR))
    for v in range(VIEWS):
        for s in range(slab):
            row = taps[1][v * slab + s : v * slab + s + 1]
            for j in range(2):
                index = base_y[j] - shift(v, s, 1)
                filter_y[v, s, :, j * lanes : (j + 1) * lanes] = lane_pick(row, index).astype(
                    jnp.bfloat16
                )

    shape = filter_w.shape
    half = shape[1] // VIEWS
    column = iota(shape, 0)
    local = iota(shape, 1) % half - MARGIN
    q = jnp.where(iota(shape, 1) < half, scalars[5, 2], scalars[6, 2])
    num = q * (2 * (depth_rank * strip + column) + 1 - width) + width
    whole = num // (2 * width)
    frac = (num - whole * (2 * width)).astype(jnp.float32) / (2.0 * width)
    filter_w[...] = lanczos(frac - (local - column - whole).astype(jnp.float32))


def slab_kernel(
    params, palette, filter_x, filter_y, own, got_a, got_b, keep, send, classed, near
):
    slab = own.shape[1]
    lanes, width = own.shape[2:]
    rows = lanes // 4
    for s in range(slab):

        def store(v, k, part):
            near[v, s, :, k * LANES : (k + 1) * LANES] = part

        voxels = jnp.concatenate(
            [got_a[s].astype(jnp.int32), got_b[s].astype(jnp.int32)], axis=0
        )
        shear_columns(voxels, palette[...], filter_x[s], classed, store)
    chunk = 2 * LANES
    for v in range(VIEWS):
        facing = params[1 + v, 3] >= 0
        for side in (slice(0, HALO), slice(HALO + width, 2 * HALO + width)):
            keep[v, side] = jnp.zeros((HALO, lanes), jnp.float32)
            send[v, side] = jnp.zeros((HALO, lanes), jnp.bfloat16)
        for k in range(width // chunk):
            for step in range(slab):
                s = jnp.where(facing, step, slab - 1 - step)
                source = jnp.concatenate(
                    [
                        own[v, s, :, k * chunk : (k + 1) * chunk],
                        near[v, s, :, k * chunk : (k + 1) * chunk],
                    ],
                    axis=0,
                )
                sheared = jnp.dot(filter_y[v, s], source, preferred_element_type=jnp.float32)
                if step == 0:
                    picture = sheared
                    continue
                through = 1.0 - picture[3 * rows :]
                picture = picture + jnp.concatenate([through] * 4, axis=0) * sheared
            turned = picture.T
            at = slice(HALO + k * chunk, HALO + (k + 1) * chunk)
            keep[v, at] = turned
            send[v, at] = turned.astype(jnp.bfloat16)


def merge_kernel(params, keep, got, out):
    strips, both, lanes = out.shape
    span = both // VIEWS
    wide = span + 2 * (HALO - MARGIN)
    rows = lanes // 4
    core = params[0, 0] % 2
    pick = 3 * rows + iota((wide, lanes), 1) % rows
    for k in range(strips):
        at = pl.ds(pl.multiple_of(k * wide + core * (wide // 2), wide // 2), wide)
        done = []
        for v in range(VIEWS):
            mine_front = (params[1 + v, 3] >= 0) == (core == 0)
            mine = keep[v, at]
            other = got[v, at].astype(jnp.float32)
            front = jnp.where(mine_front, mine, other)
            back = jnp.where(mine_front, other, mine)
            alpha = jnp.take_along_axis(front, pick, axis=1, mode="promise_in_bounds")
            merged = front + (1.0 - alpha) * back
            done.append(merged[HALO - MARGIN : HALO - MARGIN + span])
        out[k] = jnp.concatenate(done, axis=0).astype(jnp.bfloat16)


def final_kernel(params, filter_w, arrived, out):
    slabs, both, lanes = arrived.shape
    span = both // VIEWS
    rows = lanes // 4
    pick = 3 * rows + iota((span, lanes), 1) % rows
    for v in range(VIEWS):
        facing = params[1 + v, 3] >= 0
        picture = jnp.zeros((span, lanes), jnp.float32)
        through = jnp.ones((span, lanes), jnp.float32)
        for k in range(slabs):
            at = jnp.where(facing, k, slabs - 1 - k)
            part = arrived[at].astype(jnp.float32)[v * span : (v + 1) * span]
            picture = picture + through * part
            through = through * (
                1.0 - jnp.take_along_axis(part, pick, axis=1, mode="promise_in_bounds")
            )
        half = filter_w.shape[1] // VIEWS
        final = jnp.dot(
            filter_w[:, v * half : v * half + span],
            picture,
            precision=lax.Precision.HIGHEST,
            preferred_element_type=jnp.float32,
        )
        for c in range(4):
            out[v, :, c, :] = final[:, c * rows : (c + 1) * rows]


def call(kernel, outs, scratch=(), spaces=(), out_spaces=None):
    def run(*args):
        given = list(spaces) + [pltpu.VMEM] * (len(args) - len(spaces))
        where = out_spaces or jax.tree.map(lambda _: pltpu.VMEM, outs)
        return pl.pallas_call(
            kernel,
            out_shape=outs,
            in_specs=[pl.BlockSpec(memory_space=space) for space in given],
            out_specs=jax.tree.map(lambda space: pl.BlockSpec(memory_space=space), where),
            scratch_shapes=list(scratch),
            compiler_params=pltpu.CompilerParams(vmem_limit_bytes=VMEM_LIMIT),
        )(*args)

    return run


def body(volume, tf_table, view_code):
    slab, rows, width = volume.shape
    depth_size = lax.axis_size("depth")
    band_size = lax.axis_size("band")
    strip = width // depth_size
    lanes = 4 * rows
    bf16, f32, i32 = jnp.bfloat16, jnp.float32, jnp.int32
    shape = jax.ShapeDtypeStruct
    smem = (pltpu.SMEM,)
    ids = jnp.stack(
        [lax.axis_index("depth"), lax.axis_index("band"), jnp.int32(depth_size), jnp.int32(band_size)]
    ).astype(i32)
    wide = tf_table.shape[1]
    tables = jnp.concatenate(
        [tf_table]
        + [jnp.pad(part, ((0, 0), (0, wide - 4))) for part in (ids[None], view_code)]
        + [jnp.zeros((1, wide), i32)],
        axis=0,
    )
    voxels = volume.astype(bf16)
    even = lax.axis_index("band") % 2 == 0
    first = voxels[:, :HALO]
    last = voxels[:, rows - HALO :]
    send_a = jnp.where(even, last, first)
    send_b = jnp.where(even, first, last)
    got_a = lax.ppermute(send_a, "band", pairs(band_size, 0))
    got_b = lax.ppermute(send_b, "band", pairs(band_size, 1))
    params, palette, own, filter_x, filter_y, filter_w = call(
        own_kernel,
        (
            shape((1 + VIEWS, 4), i32),
            shape(tf_table.shape, f32),
            shape((VIEWS, slab, lanes, width), bf16),
            shape((slab, 2 * LANES, VIEWS * LANES), bf16),
            shape((VIEWS, slab, lanes, 2 * lanes), bf16),
            shape((strip, VIEWS * (strip + 2 * HALO)), f32),
        ),
        (pltpu.VMEM((lanes, width + LANES), bf16),),
        smem,
        (pltpu.SMEM,) + (pltpu.VMEM,) * 5,
    )(tables, tables, voxels)
    padded = (VIEWS, width + 2 * HALO, lanes)
    keep, send = call(
        slab_kernel,
        (shape(padded, f32), shape(padded, bf16)),
        (
            pltpu.VMEM((8 * HALO, width + LANES), bf16),
            pltpu.VMEM((VIEWS, slab, 8 * HALO, width), bf16),
        ),
        smem,
    )(params, palette, filter_x, filter_y, own, got_a, got_b)
    got = lax.ppermute(send, "depth", pairs(depth_size, 0))
    merged = shape((depth_size // 2, VIEWS * (strip + 2 * MARGIN), lanes), bf16)
    merged = call(merge_kernel, merged, (), smem)(params, keep, got)
    arrived = lax.all_to_all(
        merged,
        "depth",
        split_axis=0,
        concat_axis=0,
        tiled=True,
        axis_index_groups=[list(range(i, depth_size, 2)) for i in range(2)],
    )
    final = shape((VIEWS, strip, 4, rows), f32)
    return call(final_kernel, final, (), smem)(params, filter_w, arrived)


def solution(mesh):
    placed = (P("depth", "band", None), P(), P())
    return jax.shard_map(
        body, mesh=mesh, in_specs=placed, out_specs=P(None, "depth", None, "band"), check_vma=False
    )
```

```python
import jax
import jax.numpy as jnp
from jax import lax
from jax.experimental import pallas as pl
from jax.experimental.pallas import tpu as pltpu
from jax.sharding import PartitionSpec as P

VIEWS = 2
HALO = 16
MARGIN = 12
LANES = 128
CENTER = 64
FAR = 20
VMEM_LIMIT = 16 * 2**20


def sinc(t):
    angle = jnp.where(t == 0.0, 1.0, jnp.pi * t)
    return jnp.where(t == 0.0, 1.0, jnp.sin(angle) / angle)


def lanczos(offset):
    return jnp.where(jnp.abs(offset) < 3.0, sinc(offset) * sinc(offset / 3.0), 0.0)


def iota(shape, dim):
    return lax.broadcasted_iota(jnp.int32, shape, dim)


def pairs(size, first):
    out = []
    for a in range(first, size - 1, 2):
        out += [(a, a + 1), (a + 1, a)]
    return out


def lane_gather(table, index):
    numbers = lax.GatherDimensionNumbers(
        offset_dims=(),
        collapsed_slice_dims=(1,),
        start_index_map=(1,),
        operand_batching_dims=(0,),
        start_indices_batching_dims=(0,),
    )
    return lax.gather(
        table,
        index[..., None],
        numbers,
        slice_sizes=(1, 1),
        mode=lax.GatherScatterMode.PROMISE_IN_BOUNDS,
    )


def lane_pick(row, index):
    return lane_gather(jnp.broadcast_to(row, index.shape), index)


def classify(code, palette, out, k, last):
    high = code >= LANES
    low = code & (LANES - 1)
    values = []
    for c in range(4):
        value = jnp.where(
            high,
            lane_pick(palette[c : c + 1, LANES:], low),
            lane_pick(palette[c : c + 1, :LANES], low),
        )
        if k == 0:
            value = jnp.where(iota(value.shape, 1) >= CENTER, value, 0.0)
        if k == last:
            value = jnp.where(iota(value.shape, 1) < CENTER, value, 0.0)
        values.append(value)
    out[:, k * LANES : (k + 1) * LANES] = jnp.concatenate(values, axis=0).astype(jnp.bfloat16)


def shear_columns(voxels, palette, weights, classed, store):
    group, width = voxels.shape
    blocks = width // LANES
    side = jnp.zeros((group, CENTER), jnp.int32)
    voxels = jnp.concatenate([side, voxels, side], axis=1)
    for k in range(blocks + 1):
        classify(voxels[:, k * LANES : (k + 1) * LANES], palette, classed, k, blocks)
    for k in range(blocks):
        part = jnp.dot(
            classed[:, k * LANES : (k + 2) * LANES], weights, preferred_element_type=jnp.float32
        ).astype(jnp.bfloat16)
        for v in range(VIEWS):
            store(v, k, part[:, v * LANES : (v + 1) * LANES])


def own_kernel(
    scalars, tables, vol, params, palette_out, own, filter_x, filter_y, filter_w, classed
):
    slab, rows, width = vol.shape
    for i in range(1 + VIEWS):
        for j in range(4):
            params[i, j] = scalars[4 + i, j]
    depth_rank, band_rank = scalars[4, 0], scalars[4, 1]
    depth = slab * scalars[4, 2]
    height = rows * scalars[4, 3]
    strip = filter_w.shape[0]

    codes = tables[0:4].astype(jnp.float32)
    opacity = codes[3:4] / (64.0 * depth.astype(jnp.float32))
    premult = codes[0:3] / 255.0 * opacity
    palette = jnp.concatenate([premult, opacity], axis=0).astype(jnp.bfloat16).astype(jnp.float32)
    palette_out[...] = palette

    which = iota((VIEWS * slab, LANES), 0)
    lane = iota((VIEWS * slab, LANES), 1)
    place = depth_rank * slab + which % slab
    taps = []
    for column in range(2):
        q = jnp.where(which < slab, scalars[5, column], scalars[6, column])
        num = q * (2 * place + 1 - depth)
        whole = num // (2 * depth)
        frac = (num - whole * (2 * depth)).astype(jnp.float32) / (2.0 * depth.astype(jnp.float32))
        taps.append(
            lanczos(frac - (lane - CENTER - whole).astype(jnp.float32))
            .astype(jnp.bfloat16)
            .astype(jnp.float32)
        )

    base_x = iota((2 * LANES, LANES), 0) - iota((2 * LANES, LANES), 1)
    base_x = jnp.clip(base_x, FAR, LANES - 1 - FAR)
    for i in range(0, 2 * LANES, 16):
        for s in range(slab):
            for v in range(VIEWS):
                row = taps[0][v * slab + s : v * slab + s + 1]
                filter_x[s, i : i + 16, v * LANES : (v + 1) * LANES] = lane_pick(
                    row, base_x[i : i + 16]
                ).astype(jnp.bfloat16)
    for s in range(slab):

        def store(v, k, part):
            own[v, s, :, k * LANES : (k + 1) * LANES] = part

        shear_columns(vol[s].astype(jnp.int32), palette, filter_x[s], classed, store)

    lanes = 4 * rows
    to = iota((lanes, lanes), 0)
    frm = iota((lanes, lanes), 1)
    even = band_rank % 2 == 0
    start_a = jnp.where(even, rows, -MARGIN)
    start_b = jnp.where(even, -MARGIN, rows)
    base_y = []
    for each, at in ((rows, frm % rows), (2 * MARGIN, frm % (2 * MARGIN))):
        local = at
        if each != rows:
            local = jnp.where(at < MARGIN, at + start_a, at - MARGIN + start_b)
        world = local + band_rank * rows
        fits = (to // rows == frm // each) & (world >= 0) & (world < height)
        base_y.append(jnp.where(fits, local - to % rows + CENTER, FAR))
    for j in range(2):
        for i in range(0, lanes, 16):
            for v in range(VIEWS):
                for s in range(slab):
                    row = taps[1][v * slab + s : v * slab + s + 1]
                    filter_y[v, s, i : i + 16, j * lanes : (j + 1) * lanes] = lane_pick(
                        row, base_y[j][i : i + 16]
                    ).astype(jnp.bfloat16)

    shape = filter_w.shape
    half = shape[1] // VIEWS
    column = iota(shape, 0)
    local = iota(shape, 1) % half - MARGIN
    q = jnp.where(iota(shape, 1) < half, scalars[5, 2], scalars[6, 2])
    num = q * (2 * (depth_rank * strip + column) + 1 - width) + width
    whole = num // (2 * width)
    frac = (num - whole * (2 * width)).astype(jnp.float32) / (2.0 * width)
    filter_w[...] = lanczos(frac - (local - column - whole).astype(jnp.float32))


def slab_kernel(
    params, palette, filter_x, filter_y, own, got_a, got_b, keep, send, classed, near
):
    slab = own.shape[1]
    lanes, width = own.shape[2:]
    rows = lanes // 4
    fill = 8 * MARGIN
    codes_a = got_a[...].astype(jnp.int32)
    codes_b = got_b[...].astype(jnp.int32)
    for s in range(slab):
        for v in range(VIEWS):
            near[v, s, fill:] = jnp.zeros((lanes - fill, width), jnp.bfloat16)

        def store(v, k, part):
            near[v, s, :fill, k * LANES : (k + 1) * LANES] = part

        at = slice(s * MARGIN, (s + 1) * MARGIN)
        voxels = jnp.concatenate([codes_a[at], codes_b[at]], axis=0)
        shear_columns(voxels, palette[...], filter_x[s], classed, store)
    chunk = 2 * LANES
    for v in range(VIEWS):
        facing = params[1 + v, 3] >= 0
        for side in (slice(0, HALO), slice(HALO + width, 2 * HALO + width)):
            keep[v, side] = jnp.zeros((HALO, lanes), jnp.float32)
            send[v, side] = jnp.zeros((HALO, lanes), jnp.bfloat16)
        for k in range(width // chunk):
            for step in range(slab):
                s = jnp.where(facing, step, slab - 1 - step)
                source = jnp.concatenate(
                    [
                        own[v, s, :, k * chunk : (k + 1) * chunk],
                        near[v, s, :, k * chunk : (k + 1) * chunk],
                    ],
                    axis=0,
                )
                sheared = jnp.dot(filter_y[v, s], source, preferred_element_type=jnp.float32)
                if step == 0:
                    picture = sheared
                    continue
                through = 1.0 - picture[3 * rows :]
                picture = picture + jnp.concatenate([through] * 4, axis=0) * sheared
            turned = picture.T
            at = slice(HALO + k * chunk, HALO + (k + 1) * chunk)
            keep[v, at] = turned
            send[v, at] = turned.astype(jnp.bfloat16)


def merge_kernel(params, keep, got, out):
    strips, both, lanes = out.shape
    span = both // VIEWS
    wide = span + 2 * (HALO - MARGIN)
    rows = lanes // 4
    core = params[0, 0] % 2
    pick = 3 * rows + iota((wide, lanes), 1) % rows
    for k in range(strips):
        at = pl.ds(pl.multiple_of(k * wide + core * (wide // 2), wide // 2), wide)
        done = []
        for v in range(VIEWS):
            mine_front = (params[1 + v, 3] >= 0) == (core == 0)
            mine = keep[v, at]
            other = got[v, at].astype(jnp.float32)
            front = jnp.where(mine_front, mine, other)
            back = jnp.where(mine_front, other, mine)
            alpha = lane_gather(front, pick)
            merged = front + (1.0 - alpha) * back
            done.append(merged[HALO - MARGIN : HALO - MARGIN + span])
        out[k] = jnp.concatenate(done, axis=0).astype(jnp.bfloat16)


def final_kernel(params, filter_w, arrived, out):
    slabs, both, lanes = arrived.shape
    span = both // VIEWS
    rows = lanes // 4
    pick = 3 * rows + iota((span, lanes), 1) % rows
    for v in range(VIEWS):
        facing = params[1 + v, 3] >= 0
        picture = jnp.zeros((span, lanes), jnp.float32)
        through = jnp.ones((span, lanes), jnp.float32)
        for k in range(slabs):
            at = jnp.where(facing, k, slabs - 1 - k)
            part = arrived[at].astype(jnp.float32)[v * span : (v + 1) * span]
            picture = picture + through * part
            through = through * (
                1.0 - lane_gather(part, pick)
            )
        half = filter_w.shape[1] // VIEWS
        final = jnp.dot(
            filter_w[:, v * half : v * half + span],
            picture,
            precision=lax.Precision.HIGHEST,
            preferred_element_type=jnp.float32,
        )
        for c in range(4):
            out[v, :, c, :] = final[:, c * rows : (c + 1) * rows]


def call(kernel, outs, scratch=(), spaces=(), out_spaces=None):
    def run(*args):
        given = list(spaces) + [pltpu.VMEM] * (len(args) - len(spaces))
        where = out_spaces or jax.tree.map(lambda _: pltpu.VMEM, outs)
        return pl.pallas_call(
            kernel,
            out_shape=outs,
            in_specs=[pl.BlockSpec(memory_space=space) for space in given],
            out_specs=jax.tree.map(lambda space: pl.BlockSpec(memory_space=space), where),
            scratch_shapes=list(scratch),
            compiler_params=pltpu.CompilerParams(vmem_limit_bytes=VMEM_LIMIT),
        )(*args)

    return run


def body(volume, tf_table, view_code):
    slab, rows, width = volume.shape
    depth_size = lax.axis_size("depth")
    band_size = lax.axis_size("band")
    strip = width // depth_size
    lanes = 4 * rows
    bf16, f32, i32 = jnp.bfloat16, jnp.float32, jnp.int32
    shape = jax.ShapeDtypeStruct
    smem = (pltpu.SMEM,)
    ids = jnp.stack(
        [lax.axis_index("depth"), lax.axis_index("band"), jnp.int32(depth_size), jnp.int32(band_size)]
    ).astype(i32)
    wide = tf_table.shape[1]
    tables = jnp.concatenate(
        [tf_table]
        + [jnp.pad(part, ((0, 0), (0, wide - 4))) for part in (ids[None], view_code)]
        + [jnp.zeros((1, wide), i32)],
        axis=0,
    )
    voxels = volume.astype(bf16)
    even = lax.axis_index("band") % 2 == 0
    first = voxels[:, :MARGIN].reshape(slab * MARGIN, width)
    last = voxels[:, rows - MARGIN :].reshape(slab * MARGIN, width)
    send_a = jnp.where(even, last, first)
    send_b = jnp.where(even, first, last)
    got_a = lax.ppermute(send_a, "band", pairs(band_size, 0))
    got_b = lax.ppermute(send_b, "band", pairs(band_size, 1))
    params, palette, own, filter_x, filter_y, filter_w = call(
        own_kernel,
        (
            shape((1 + VIEWS, 4), i32),
            shape(tf_table.shape, f32),
            shape((VIEWS, slab, lanes, width), bf16),
            shape((slab, 2 * LANES, VIEWS * LANES), bf16),
            shape((VIEWS, slab, lanes, 2 * lanes), bf16),
            shape((strip, VIEWS * (strip + 2 * HALO)), f32),
        ),
        (pltpu.VMEM((lanes, width + LANES), bf16),),
        smem,
        (pltpu.SMEM,) + (pltpu.VMEM,) * 5,
    )(tables, tables, voxels)
    padded = (VIEWS, width + 2 * HALO, lanes)
    keep, send = call(
        slab_kernel,
        (shape(padded, f32), shape(padded, bf16)),
        (
            pltpu.VMEM((8 * MARGIN, width + LANES), bf16),
            pltpu.VMEM((VIEWS, slab, lanes, width), bf16),
        ),
        smem,
    )(params, palette, filter_x, filter_y, own, got_a, got_b)
    got = lax.ppermute(send, "depth", pairs(depth_size, 0))
    merged = shape((depth_size // 2, VIEWS * (strip + 2 * MARGIN), lanes), bf16)
    merged = call(merge_kernel, merged, (), smem)(params, keep, got)
    arrived = lax.all_to_all(
        merged,
        "depth",
        split_axis=0,
        concat_axis=0,
        tiled=True,
        axis_index_groups=[list(range(i, depth_size, 2)) for i in range(2)],
    )
    final = shape((VIEWS, strip, 4, rows), f32)
    return call(final_kernel, final, (), smem)(params, filter_w, arrived)


def solution(mesh):
    placed = (P("depth", "band", None), P(), P())
    return jax.shard_map(
        body, mesh=mesh, in_specs=placed, out_specs=P(None, "depth", None, "band"), check_vma=False
    )
```

```python
import functools

import jax
import jax.numpy as jnp
from jax import lax
from jax.experimental import pallas as pl
from jax.experimental.pallas import tpu as pltpu
from jax.sharding import PartitionSpec as P

VIEWS = 2
HALO = 16
MARGIN = 12
LANES = 128
CENTER = 64
FAR = 20
VMEM_LIMIT = 16 * 2**20


def sinc(t):
    angle = jnp.where(t == 0.0, 1.0, jnp.pi * t)
    return jnp.where(t == 0.0, 1.0, jnp.sin(angle) / angle)


def lanczos(offset):
    return jnp.where(jnp.abs(offset) < 3.0, sinc(offset) * sinc(offset / 3.0), 0.0)


def iota(shape, dim):
    return lax.broadcasted_iota(jnp.int32, shape, dim)


def pairs(size, first):
    out = []
    for a in range(first, size - 1, 2):
        out += [(a, a + 1), (a + 1, a)]
    return out


def lane_gather(table, index):
    numbers = lax.GatherDimensionNumbers(
        offset_dims=(),
        collapsed_slice_dims=(1,),
        start_index_map=(1,),
        operand_batching_dims=(0,),
        start_indices_batching_dims=(0,),
    )
    return lax.gather(
        table,
        index[..., None],
        numbers,
        slice_sizes=(1, 1),
        mode=lax.GatherScatterMode.PROMISE_IN_BOUNDS,
    )


def lane_pick(row, index):
    return lane_gather(jnp.broadcast_to(row, index.shape), index)


def classify(code, palette, out, k, last):
    high = code >= LANES
    low = code & (LANES - 1)
    values = []
    for c in range(4):
        value = jnp.where(
            high,
            lane_pick(palette[c : c + 1, LANES:], low),
            lane_pick(palette[c : c + 1, :LANES], low),
        )
        if k == 0:
            value = jnp.where(iota(value.shape, 1) >= CENTER, value, 0.0)
        if k == last:
            value = jnp.where(iota(value.shape, 1) < CENTER, value, 0.0)
        values.append(value)
    out[:, k * LANES : (k + 1) * LANES] = jnp.concatenate(values, axis=0).astype(jnp.bfloat16)


def shear_columns(voxels, palette, weights, classed, store):
    group, width = voxels.shape
    blocks = width // LANES
    side = jnp.zeros((group, CENTER), jnp.int32)
    voxels = jnp.concatenate([side, voxels, side], axis=1)
    for k in range(blocks + 1):
        classify(voxels[:, k * LANES : (k + 1) * LANES], palette, classed, k, blocks)
    for k in range(blocks):
        part = jnp.dot(
            classed[:, k * LANES : (k + 2) * LANES], weights, preferred_element_type=jnp.float32
        ).astype(jnp.bfloat16)
        for v in range(VIEWS):
            store(v, k, part[:, v * LANES : (v + 1) * LANES])


def own_kernel(
    depth, height, tables, vol, palette_out, own, filter_x, filter_y, filter_w, classed
):
    slab, rows, width = vol.shape
    depth_rank, band_rank = tables[4:5, 0:1], tables[4:5, 1:2]
    strip = filter_w.shape[0]

    codes = tables[0:4].astype(jnp.float32)
    opacity = codes[3:4] / (64.0 * depth)
    premult = codes[0:3] / 255.0 * opacity
    palette = jnp.concatenate([premult, opacity], axis=0).astype(jnp.bfloat16).astype(jnp.float32)
    palette_out[...] = palette

    which = iota((VIEWS * slab, LANES), 0)
    lane = iota((VIEWS * slab, LANES), 1)
    place = depth_rank * slab + which % slab
    taps = []
    for column in range(2):
        q = jnp.where(which < slab, tables[5:6, column : column + 1], tables[6:7, column : column + 1])
        num = q * (2 * place + 1 - depth)
        whole = num // (2 * depth)
        frac = (num - whole * (2 * depth)).astype(jnp.float32) / (2.0 * depth)
        taps.append(
            lanczos(frac - (lane - CENTER - whole).astype(jnp.float32))
            .astype(jnp.bfloat16)
            .astype(jnp.float32)
        )

    base_x = iota((2 * LANES, LANES), 0) - iota((2 * LANES, LANES), 1)
    base_x = jnp.clip(base_x, FAR, LANES - 1 - FAR)
    for i in range(0, 2 * LANES, 16):
        for s in range(slab):
            for v in range(VIEWS):
                row = taps[0][v * slab + s : v * slab + s + 1]
                filter_x[s, i : i + 16, v * LANES : (v + 1) * LANES] = lane_pick(
                    row, base_x[i : i + 16]
                ).astype(jnp.bfloat16)
    for s in range(slab):

        def store(v, k, part):
            own[v, s, :, k * LANES : (k + 1) * LANES] = part

        shear_columns(vol[s].astype(jnp.int32), palette, filter_x[s], classed, store)

    lanes = 4 * rows
    to = iota((lanes, lanes), 0)
    frm = iota((lanes, lanes), 1)
    even = band_rank % 2 == 0
    start_a = jnp.where(even, rows, -MARGIN)
    start_b = jnp.where(even, -MARGIN, rows)
    base_y = []
    for each, at in ((rows, frm % rows), (2 * MARGIN, frm % (2 * MARGIN))):
        local = at
        if each != rows:
            local = jnp.where(at < MARGIN, at + start_a, at - MARGIN + start_b)
        world = local + band_rank * rows
        fits = (to // rows == frm // each) & (world >= 0) & (world < height)
        base_y.append(jnp.where(fits, local - to % rows + CENTER, FAR))
    for j in range(2):
        for i in range(0, lanes, 16):
            for v in range(VIEWS):
                for s in range(slab):
                    row = taps[1][v * slab + s : v * slab + s + 1]
                    filter_y[v, s, i : i + 16, j * lanes : (j + 1) * lanes] = lane_pick(
                        row, base_y[j][i : i + 16]
                    ).astype(jnp.bfloat16)

    shape = filter_w.shape
    half = shape[1] // VIEWS
    column = iota(shape, 0)
    local = iota(shape, 1) % half - MARGIN
    q = jnp.where(iota(shape, 1) < half, tables[5:6, 2:3], tables[6:7, 2:3])
    num = q * (2 * (depth_rank * strip + column) + 1 - width) + width
    whole = num // (2 * width)
    frac = (num - whole * (2 * width)).astype(jnp.float32) / (2.0 * width)
    filter_w[...] = lanczos(frac - (local - column - whole).astype(jnp.float32))


def slab_kernel(
    tables, palette, filter_x, filter_y, own, got_a, got_b, keep, send, classed, near, params, sem
):
    scalars = pltpu.make_async_copy(tables, params, sem)
    scalars.start()
    slab = own.shape[1]
    lanes, width = own.shape[2:]
    rows = lanes // 4
    fill = 8 * MARGIN
    codes_a = got_a[...].astype(jnp.int32)
    codes_b = got_b[...].astype(jnp.int32)
    for s in range(slab):
        for v in range(VIEWS):
            near[v, s, fill:] = jnp.zeros((lanes - fill, width), jnp.bfloat16)

        def store(v, k, part):
            near[v, s, :fill, k * LANES : (k + 1) * LANES] = part

        at = slice(s * MARGIN, (s + 1) * MARGIN)
        voxels = jnp.concatenate([codes_a[at], codes_b[at]], axis=0)
        shear_columns(voxels, palette[...], filter_x[s], classed, store)
    scalars.wait()
    chunk = 2 * LANES
    for v in range(VIEWS):
        facing = params[5 + v, 3] >= 0
        for side in (slice(0, HALO), slice(HALO + width, 2 * HALO + width)):
            keep[v, side] = jnp.zeros((HALO, lanes), jnp.float32)
            send[v, side] = jnp.zeros((HALO, lanes), jnp.bfloat16)
        for k in range(width // chunk):
            for step in range(slab):
                s = jnp.where(facing, step, slab - 1 - step)
                source = jnp.concatenate(
                    [
                        own[v, s, :, k * chunk : (k + 1) * chunk],
                        near[v, s, :, k * chunk : (k + 1) * chunk],
                    ],
                    axis=0,
                )
                sheared = jnp.dot(filter_y[v, s], source, preferred_element_type=jnp.float32)
                if step == 0:
                    picture = sheared
                    continue
                through = 1.0 - picture[3 * rows :]
                picture = picture + jnp.concatenate([through] * 4, axis=0) * sheared
            turned = picture.T
            at = slice(HALO + k * chunk, HALO + (k + 1) * chunk)
            keep[v, at] = turned
            send[v, at] = turned.astype(jnp.bfloat16)


def merge_kernel(params, keep, got, out):
    strips, both, lanes = out.shape
    span = both // VIEWS
    wide = span + 2 * (HALO - MARGIN)
    rows = lanes // 4
    core = params[4, 0] % 2
    pick = 3 * rows + iota((wide, lanes), 1) % rows
    for k in range(strips):
        at = pl.ds(pl.multiple_of(k * wide + core * (wide // 2), wide // 2), wide)
        done = []
        for v in range(VIEWS):
            mine_front = (params[5 + v, 3] >= 0) == (core == 0)
            mine = keep[v, at]
            other = got[v, at].astype(jnp.float32)
            front = jnp.where(mine_front, mine, other)
            back = jnp.where(mine_front, other, mine)
            alpha = lane_gather(front, pick)
            merged = front + (1.0 - alpha) * back
            done.append(merged[HALO - MARGIN : HALO - MARGIN + span])
        out[k] = jnp.concatenate(done, axis=0).astype(jnp.bfloat16)


def final_kernel(params, filter_w, arrived, out):
    slabs, both, lanes = arrived.shape
    span = both // VIEWS
    rows = lanes // 4
    pick = 3 * rows + iota((span, lanes), 1) % rows
    for v in range(VIEWS):
        facing = params[5 + v, 3] >= 0
        picture = jnp.zeros((span, lanes), jnp.float32)
        through = jnp.ones((span, lanes), jnp.float32)
        for k in range(slabs):
            at = jnp.where(facing, k, slabs - 1 - k)
            part = arrived[at].astype(jnp.float32)[v * span : (v + 1) * span]
            picture = picture + through * part
            through = through * (
                1.0 - lane_gather(part, pick)
            )
        half = filter_w.shape[1] // VIEWS
        final = jnp.dot(
            filter_w[:, v * half : v * half + span],
            picture,
            precision=lax.Precision.HIGHEST,
            preferred_element_type=jnp.float32,
        )
        for c in range(4):
            out[v, :, c, :] = final[:, c * rows : (c + 1) * rows]


def call(kernel, outs, scratch=(), spaces=(), out_spaces=None):
    def run(*args):
        given = list(spaces) + [pltpu.VMEM] * (len(args) - len(spaces))
        where = out_spaces or jax.tree.map(lambda _: pltpu.VMEM, outs)
        return pl.pallas_call(
            kernel,
            out_shape=outs,
            in_specs=[pl.BlockSpec(memory_space=space) for space in given],
            out_specs=jax.tree.map(lambda space: pl.BlockSpec(memory_space=space), where),
            scratch_shapes=list(scratch),
            compiler_params=pltpu.CompilerParams(vmem_limit_bytes=VMEM_LIMIT),
        )(*args)

    return run


def body(volume, tf_table, view_code):
    slab, rows, width = volume.shape
    depth_size = lax.axis_size("depth")
    band_size = lax.axis_size("band")
    strip = width // depth_size
    lanes = 4 * rows
    bf16, f32, i32 = jnp.bfloat16, jnp.float32, jnp.int32
    shape = jax.ShapeDtypeStruct
    smem = (pltpu.SMEM,)
    ids = jnp.stack(
        [lax.axis_index("depth"), lax.axis_index("band"), jnp.int32(depth_size), jnp.int32(band_size)]
    ).astype(i32)
    wide = tf_table.shape[1]
    tables = jnp.concatenate(
        [tf_table]
        + [jnp.pad(part, ((0, 0), (0, wide - 4))) for part in (ids[None], view_code)]
        + [jnp.zeros((1, wide), i32)],
        axis=0,
    )
    voxels = volume.astype(bf16)
    even = lax.axis_index("band") % 2 == 0
    first = voxels[:, :MARGIN].reshape(slab * MARGIN, width)
    last = voxels[:, rows - MARGIN :].reshape(slab * MARGIN, width)
    send_a = jnp.where(even, last, first)
    send_b = jnp.where(even, first, last)
    got_a = lax.ppermute(send_a, "band", pairs(band_size, 0))
    got_b = lax.ppermute(send_b, "band", pairs(band_size, 1))
    palette, own, filter_x, filter_y, filter_w = call(
        functools.partial(own_kernel, slab * depth_size, rows * band_size),
        (
            shape(tf_table.shape, f32),
            shape((VIEWS, slab, lanes, width), bf16),
            shape((slab, 2 * LANES, VIEWS * LANES), bf16),
            shape((VIEWS, slab, lanes, 2 * lanes), bf16),
            shape((strip, VIEWS * (strip + 2 * HALO)), f32),
        ),
        (pltpu.VMEM((lanes, width + LANES), bf16),),
    )(tables, voxels)
    padded = (VIEWS, width + 2 * HALO, lanes)
    keep, send = call(
        slab_kernel,
        (shape(padded, f32), shape(padded, bf16)),
        (
            pltpu.VMEM((8 * MARGIN, width + LANES), bf16),
            pltpu.VMEM((VIEWS, slab, lanes, width), bf16),
            pltpu.SMEM(tables.shape, i32),
            pltpu.SemaphoreType.DMA(()),
        ),
        (pl.ANY,),
    )(tables, palette, filter_x, filter_y, own, got_a, got_b)
    got = lax.ppermute(send, "depth", pairs(depth_size, 0))
    merged = shape((depth_size // 2, VIEWS * (strip + 2 * MARGIN), lanes), bf16)
    merged = call(merge_kernel, merged, (), smem)(tables, keep, got)
    arrived = lax.all_to_all(
        merged,
        "depth",
        split_axis=0,
        concat_axis=0,
        tiled=True,
        axis_index_groups=[list(range(i, depth_size, 2)) for i in range(2)],
    )
    final = shape((VIEWS, strip, 4, rows), f32)
    return call(final_kernel, final, (), smem)(tables, filter_w, arrived)


def solution(mesh):
    placed = (P("depth", "band", None), P(), P())
    return jax.shard_map(
        body, mesh=mesh, in_specs=placed, out_specs=P(None, "depth", None, "band"), check_vma=False
    )
```

```python
import functools

import jax
import jax.numpy as jnp
from jax import lax
from jax.experimental import pallas as pl
from jax.experimental.pallas import tpu as pltpu
from jax.sharding import PartitionSpec as P

VIEWS = 2
HALO = 16
MARGIN = 12
LANES = 128
CENTER = 64
FAR = 20
VMEM_LIMIT = 16 * 2**20


def sinc(t):
    angle = jnp.where(t == 0.0, 1.0, jnp.pi * t)
    return jnp.where(t == 0.0, 1.0, jnp.sin(angle) / angle)


def lanczos(offset):
    return jnp.where(jnp.abs(offset) < 3.0, sinc(offset) * sinc(offset / 3.0), 0.0)


def iota(shape, dim):
    return lax.broadcasted_iota(jnp.int32, shape, dim)


def pairs(size, first):
    out = []
    for a in range(first, size - 1, 2):
        out += [(a, a + 1), (a + 1, a)]
    return out


def lane_gather(table, index):
    numbers = lax.GatherDimensionNumbers(
        offset_dims=(),
        collapsed_slice_dims=(1,),
        start_index_map=(1,),
        operand_batching_dims=(0,),
        start_indices_batching_dims=(0,),
    )
    return lax.gather(
        table,
        index[..., None],
        numbers,
        slice_sizes=(1, 1),
        mode=lax.GatherScatterMode.PROMISE_IN_BOUNDS,
    )


def lane_pick(row, index):
    return lane_gather(jnp.broadcast_to(row, index.shape), index)


def classify(code, palette, out, k, last):
    high = code >= LANES
    low = code & (LANES - 1)
    values = []
    for c in range(4):
        value = jnp.where(
            high,
            lane_pick(palette[c : c + 1, LANES:], low),
            lane_pick(palette[c : c + 1, :LANES], low),
        )
        if k == 0:
            value = jnp.where(iota(value.shape, 1) >= CENTER, value, 0.0)
        if k == last:
            value = jnp.where(iota(value.shape, 1) < CENTER, value, 0.0)
        values.append(value)
    out[:, k * LANES : (k + 1) * LANES] = jnp.concatenate(values, axis=0).astype(jnp.bfloat16)


def shear_columns(voxels, palette, weights, classed, store):
    group, width = voxels.shape
    blocks = width // LANES
    side = jnp.zeros((group, CENTER), jnp.int32)
    voxels = jnp.concatenate([side, voxels, side], axis=1)
    for k in range(blocks + 1):
        classify(voxels[:, k * LANES : (k + 1) * LANES], palette, classed, k, blocks)
    for k in range(blocks):
        part = jnp.dot(
            classed[:, k * LANES : (k + 2) * LANES], weights, preferred_element_type=jnp.float32
        ).astype(jnp.bfloat16)
        for v in range(VIEWS):
            store(v, k, part[:, v * LANES : (v + 1) * LANES])


def own_kernel(
    depth, height, tables, vol, palette_out, own, filter_x, filter_y, filter_w, classed
):
    slab, rows, width = vol.shape
    depth_rank, band_rank = tables[4:5, 0:1], tables[4:5, 1:2]
    strip = filter_w.shape[0]

    codes = tables[0:4].astype(jnp.float32)
    opacity = codes[3:4] / (64.0 * depth)
    premult = codes[0:3] / 255.0 * opacity
    palette = jnp.concatenate([premult, opacity], axis=0).astype(jnp.bfloat16).astype(jnp.float32)
    palette_out[...] = palette

    which = iota((VIEWS * slab, LANES), 0)
    lane = iota((VIEWS * slab, LANES), 1)
    place = depth_rank * slab + which % slab
    taps = []
    for column in range(2):
        q = jnp.where(which < slab, tables[5:6, column : column + 1], tables[6:7, column : column + 1])
        num = q * (2 * place + 1 - depth)
        whole = num // (2 * depth)
        frac = (num - whole * (2 * depth)).astype(jnp.float32) / (2.0 * depth)
        taps.append(
            lanczos(frac - (lane - CENTER - whole).astype(jnp.float32))
            .astype(jnp.bfloat16)
            .astype(jnp.float32)
        )

    base_x = iota((2 * LANES, LANES), 0) - iota((2 * LANES, LANES), 1)
    base_x = jnp.clip(base_x, FAR, LANES - 1 - FAR)
    for i in range(0, 2 * LANES, 16):
        for s in range(slab):
            for v in range(VIEWS):
                row = taps[0][v * slab + s : v * slab + s + 1]
                filter_x[s, i : i + 16, v * LANES : (v + 1) * LANES] = lane_pick(
                    row, base_x[i : i + 16]
                ).astype(jnp.bfloat16)
    for s in range(slab):

        def store(v, k, part):
            own[v, s, :, k * LANES : (k + 1) * LANES] = part

        shear_columns(vol[s].astype(jnp.int32), palette, filter_x[s], classed, store)

    lanes = 4 * rows
    to = iota((lanes, lanes), 0)
    frm = iota((lanes, lanes), 1)
    even = band_rank % 2 == 0
    start_a = jnp.where(even, rows, -MARGIN)
    start_b = jnp.where(even, -MARGIN, rows)
    base_y = []
    for each, at in ((rows, frm % rows), (2 * MARGIN, frm % (2 * MARGIN))):
        local = at
        if each != rows:
            local = jnp.where(at < MARGIN, at + start_a, at - MARGIN + start_b)
        world = local + band_rank * rows
        fits = (to // rows == frm // each) & (world >= 0) & (world < height)
        base_y.append(jnp.where(fits, local - to % rows + CENTER, FAR))
    for j in range(2):
        for i in range(0, lanes, 16):
            for v in range(VIEWS):
                for s in range(slab):
                    row = taps[1][v * slab + s : v * slab + s + 1]
                    filter_y[v, s, i : i + 16, j * lanes : (j + 1) * lanes] = lane_pick(
                        row, base_y[j][i : i + 16]
                    ).astype(jnp.bfloat16)

    shape = filter_w.shape
    half = shape[1] // VIEWS
    column = iota(shape, 0)
    local = iota(shape, 1) % half - MARGIN
    q = jnp.where(iota(shape, 1) < half, tables[5:6, 2:3], tables[6:7, 2:3])
    num = q * (2 * (depth_rank * strip + column) + 1 - width) + width
    whole = num // (2 * width)
    frac = (num - whole * (2 * width)).astype(jnp.float32) / (2.0 * width)
    filter_w[...] = lanczos(frac - (local - column - whole).astype(jnp.float32))


def slab_kernel(
    tables, palette, filter_x, filter_y, own, got_a, got_b, keep, send, classed, near, params, sem
):
    scalars = pltpu.make_async_copy(tables, params, sem)
    scalars.start()
    slab = own.shape[1]
    lanes, width = own.shape[2:]
    rows = lanes // 4
    fill = 8 * MARGIN
    codes_a = got_a[...].astype(jnp.int32)
    codes_b = got_b[...].astype(jnp.int32)
    for s in range(slab):
        for v in range(VIEWS):
            near[v, s, fill:] = jnp.zeros((lanes - fill, width), jnp.bfloat16)

        def store(v, k, part):
            near[v, s, :fill, k * LANES : (k + 1) * LANES] = part

        at = slice(s * MARGIN, (s + 1) * MARGIN)
        voxels = jnp.concatenate([codes_a[at], codes_b[at]], axis=0)
        shear_columns(voxels, palette[...], filter_x[s], classed, store)
    scalars.wait()
    chunk = 2 * LANES
    for v in range(VIEWS):
        facing = params[5 + v, 3] >= 0
        for side in (slice(0, HALO), slice(HALO + width, 2 * HALO + width)):
            keep[v, side] = jnp.zeros((HALO, lanes), jnp.float32)
            send[v, side] = jnp.zeros((HALO, lanes), jnp.bfloat16)
        for k in range(width // chunk):
            for step in range(slab):
                s = jnp.where(facing, step, slab - 1 - step)
                source = jnp.concatenate(
                    [
                        own[v, s, :, k * chunk : (k + 1) * chunk],
                        near[v, s, :, k * chunk : (k + 1) * chunk],
                    ],
                    axis=0,
                )
                sheared = jnp.dot(filter_y[v, s], source, preferred_element_type=jnp.float32)
                if step == 0:
                    picture = sheared
                    continue
                through = 1.0 - picture[3 * rows :]
                picture = picture + jnp.concatenate([through] * 4, axis=0) * sheared
            turned = picture.T
            at = slice(HALO + k * chunk, HALO + (k + 1) * chunk)
            keep[v, at] = turned
            send[v, at] = turned.astype(jnp.bfloat16)


def merge_kernel(tables, keep, got, out):
    strips, both, lanes = out.shape
    span = both // VIEWS
    wide = span + 2 * (HALO - MARGIN)
    rows = lanes // 4
    shape = (wide, lanes)
    core = jnp.broadcast_to(tables[4:5, 0:1] % 2, shape)
    second = core == 1
    pick = 3 * rows + iota(shape, 1) % rows
    forward = [
        jnp.broadcast_to((tables[5 + v : 6 + v, 3:4] >= 0).astype(jnp.int32), shape)
        for v in range(VIEWS)
    ]
    for k in range(strips):
        low = slice(k * wide, (k + 1) * wide)
        high = slice(k * wide + wide // 2, (k + 1) * wide + wide // 2)
        done = []
        for v in range(VIEWS):
            mine_front = forward[v] + core == 1
            mine = jnp.where(second, keep[v, high], keep[v, low])
            other = jnp.where(second, got[v, high], got[v, low]).astype(jnp.float32)
            front = jnp.where(mine_front, mine, other)
            back = jnp.where(mine_front, other, mine)
            merged = front + (1.0 - lane_gather(front, pick)) * back
            done.append(merged[HALO - MARGIN : HALO - MARGIN + span])
        out[k] = jnp.concatenate(done, axis=0).astype(jnp.bfloat16)


def final_kernel(params, filter_w, arrived, out):
    slabs, both, lanes = arrived.shape
    span = both // VIEWS
    rows = lanes // 4
    pick = 3 * rows + iota((span, lanes), 1) % rows
    for v in range(VIEWS):
        facing = params[5 + v, 3] >= 0
        picture = jnp.zeros((span, lanes), jnp.float32)
        through = jnp.ones((span, lanes), jnp.float32)
        for k in range(slabs):
            at = jnp.where(facing, k, slabs - 1 - k)
            part = arrived[at].astype(jnp.float32)[v * span : (v + 1) * span]
            picture = picture + through * part
            through = through * (
                1.0 - lane_gather(part, pick)
            )
        half = filter_w.shape[1] // VIEWS
        final = jnp.dot(
            filter_w[:, v * half : v * half + span],
            picture,
            precision=lax.Precision.HIGHEST,
            preferred_element_type=jnp.float32,
        )
        for c in range(4):
            out[v, :, c, :] = final[:, c * rows : (c + 1) * rows]


def call(kernel, outs, scratch=(), spaces=(), out_spaces=None):
    def run(*args):
        given = list(spaces) + [pltpu.VMEM] * (len(args) - len(spaces))
        where = out_spaces or jax.tree.map(lambda _: pltpu.VMEM, outs)
        return pl.pallas_call(
            kernel,
            out_shape=outs,
            in_specs=[pl.BlockSpec(memory_space=space) for space in given],
            out_specs=jax.tree.map(lambda space: pl.BlockSpec(memory_space=space), where),
            scratch_shapes=list(scratch),
            compiler_params=pltpu.CompilerParams(vmem_limit_bytes=VMEM_LIMIT),
        )(*args)

    return run


def body(volume, tf_table, view_code):
    slab, rows, width = volume.shape
    depth_size = lax.axis_size("depth")
    band_size = lax.axis_size("band")
    strip = width // depth_size
    lanes = 4 * rows
    bf16, f32, i32 = jnp.bfloat16, jnp.float32, jnp.int32
    shape = jax.ShapeDtypeStruct
    smem = (pltpu.SMEM,)
    ids = jnp.stack(
        [lax.axis_index("depth"), lax.axis_index("band"), jnp.int32(depth_size), jnp.int32(band_size)]
    ).astype(i32)
    wide = tf_table.shape[1]
    tables = jnp.concatenate(
        [tf_table]
        + [jnp.pad(part, ((0, 0), (0, wide - 4))) for part in (ids[None], view_code)]
        + [jnp.zeros((1, wide), i32)],
        axis=0,
    )
    voxels = volume.astype(bf16)
    even = lax.axis_index("band") % 2 == 0
    first = voxels[:, :MARGIN].reshape(slab * MARGIN, width)
    last = voxels[:, rows - MARGIN :].reshape(slab * MARGIN, width)
    send_a = jnp.where(even, last, first)
    send_b = jnp.where(even, first, last)
    got_a = lax.ppermute(send_a, "band", pairs(band_size, 0))
    got_b = lax.ppermute(send_b, "band", pairs(band_size, 1))
    palette, own, filter_x, filter_y, filter_w = call(
        functools.partial(own_kernel, slab * depth_size, rows * band_size),
        (
            shape(tf_table.shape, f32),
            shape((VIEWS, slab, lanes, width), bf16),
            shape((slab, 2 * LANES, VIEWS * LANES), bf16),
            shape((VIEWS, slab, lanes, 2 * lanes), bf16),
            shape((strip, VIEWS * (strip + 2 * HALO)), f32),
        ),
        (pltpu.VMEM((lanes, width + LANES), bf16),),
    )(tables, voxels)
    padded = (VIEWS, width + 2 * HALO, lanes)
    keep, send = call(
        slab_kernel,
        (shape(padded, f32), shape(padded, bf16)),
        (
            pltpu.VMEM((8 * MARGIN, width + LANES), bf16),
            pltpu.VMEM((VIEWS, slab, lanes, width), bf16),
            pltpu.SMEM(tables.shape, i32),
            pltpu.SemaphoreType.DMA(()),
        ),
        (pl.ANY,),
    )(tables, palette, filter_x, filter_y, own, got_a, got_b)
    got = lax.ppermute(send, "depth", pairs(depth_size, 0))
    merged = shape((depth_size // 2, VIEWS * (strip + 2 * MARGIN), lanes), bf16)
    merged = call(merge_kernel, merged)(tables, keep, got)
    arrived = lax.all_to_all(
        merged,
        "depth",
        split_axis=0,
        concat_axis=0,
        tiled=True,
        axis_index_groups=[list(range(i, depth_size, 2)) for i in range(2)],
    )
    final = shape((VIEWS, strip, 4, rows), f32)
    return call(final_kernel, final, (), smem)(tables, filter_w, arrived)


def solution(mesh):
    placed = (P("depth", "band", None), P(), P())
    return jax.shard_map(
        body, mesh=mesh, in_specs=placed, out_specs=P(None, "depth", None, "band"), check_vma=False
    )
```

```python
import functools

import jax
import jax.numpy as jnp
from jax import lax
from jax.experimental import pallas as pl
from jax.experimental.pallas import tpu as pltpu
from jax.sharding import PartitionSpec as P

VIEWS = 2
HALO = 16
MARGIN = 12
LANES = 128
CENTER = 64
FAR = 20
VMEM_LIMIT = 16 * 2**20


def sinc(t):
    angle = jnp.where(t == 0.0, 1.0, jnp.pi * t)
    return jnp.where(t == 0.0, 1.0, jnp.sin(angle) / angle)


def lanczos(offset):
    return jnp.where(jnp.abs(offset) < 3.0, sinc(offset) * sinc(offset / 3.0), 0.0)


def iota(shape, dim):
    return lax.broadcasted_iota(jnp.int32, shape, dim)


def pairs(size, first):
    out = []
    for a in range(first, size - 1, 2):
        out += [(a, a + 1), (a + 1, a)]
    return out


def lane_gather(table, index):
    numbers = lax.GatherDimensionNumbers(
        offset_dims=(),
        collapsed_slice_dims=(1,),
        start_index_map=(1,),
        operand_batching_dims=(0,),
        start_indices_batching_dims=(0,),
    )
    return lax.gather(
        table,
        index[..., None],
        numbers,
        slice_sizes=(1, 1),
        mode=lax.GatherScatterMode.PROMISE_IN_BOUNDS,
    )


def lane_pick(row, index):
    return lane_gather(jnp.broadcast_to(row, index.shape), index)


def classify(code, palette, out, k, last):
    high = code >= LANES
    low = code & (LANES - 1)
    values = []
    for c in range(4):
        value = jnp.where(
            high,
            lane_pick(palette[c : c + 1, LANES:], low),
            lane_pick(palette[c : c + 1, :LANES], low),
        )
        if k == 0:
            value = jnp.where(iota(value.shape, 1) >= CENTER, value, 0.0)
        if k == last:
            value = jnp.where(iota(value.shape, 1) < CENTER, value, 0.0)
        values.append(value)
    out[:, k * LANES : (k + 1) * LANES] = jnp.concatenate(values, axis=0).astype(jnp.bfloat16)


def shear_columns(voxels, palette, weights, classed, store):
    group, width = voxels.shape
    blocks = width // LANES
    side = jnp.zeros((group, CENTER), jnp.int32)
    voxels = jnp.concatenate([side, voxels, side], axis=1)
    for k in range(blocks + 1):
        classify(voxels[:, k * LANES : (k + 1) * LANES], palette, classed, k, blocks)
    for k in range(blocks):
        part = jnp.dot(
            classed[:, k * LANES : (k + 2) * LANES], weights, preferred_element_type=jnp.float32
        ).astype(jnp.bfloat16)
        for v in range(VIEWS):
            store(v, k, part[:, v * LANES : (v + 1) * LANES])


def own_kernel(
    depth, height, tables, vol, palette_out, own, filter_x, filter_y, filter_w, classed
):
    slab, rows, width = vol.shape
    depth_rank, band_rank = tables[4:5, 0:1], tables[4:5, 1:2]
    strip = filter_w.shape[0]

    codes = tables[0:4].astype(jnp.float32)
    opacity = codes[3:4] / (64.0 * depth)
    premult = codes[0:3] / 255.0 * opacity
    palette = jnp.concatenate([premult, opacity], axis=0).astype(jnp.bfloat16).astype(jnp.float32)
    palette_out[...] = palette

    which = iota((VIEWS * slab, LANES), 0)
    lane = iota((VIEWS * slab, LANES), 1)
    place = depth_rank * slab + which % slab
    taps = []
    for column in range(2):
        q = jnp.where(which < slab, tables[5:6, column : column + 1], tables[6:7, column : column + 1])
        num = q * (2 * place + 1 - depth)
        whole = num // (2 * depth)
        frac = (num - whole * (2 * depth)).astype(jnp.float32) / (2.0 * depth)
        taps.append(
            lanczos(frac - (lane - CENTER - whole).astype(jnp.float32))
            .astype(jnp.bfloat16)
            .astype(jnp.float32)
        )

    base_x = iota((2 * LANES, LANES), 0) - iota((2 * LANES, LANES), 1)
    base_x = jnp.clip(base_x, FAR, LANES - 1 - FAR)
    for i in range(0, 2 * LANES, 16):
        for s in range(slab):
            for v in range(VIEWS):
                row = taps[0][v * slab + s : v * slab + s + 1]
                filter_x[s, i : i + 16, v * LANES : (v + 1) * LANES] = lane_pick(
                    row, base_x[i : i + 16]
                ).astype(jnp.bfloat16)
    for s in range(slab):

        def store(v, k, part):
            own[v, s, :, k * LANES : (k + 1) * LANES] = part

        shear_columns(vol[s].astype(jnp.int32), palette, filter_x[s], classed, store)

    lanes = 4 * rows
    to = iota((lanes, lanes), 0)
    frm = iota((lanes, lanes), 1)
    even = band_rank % 2 == 0
    start_a = jnp.where(even, rows, -MARGIN)
    start_b = jnp.where(even, -MARGIN, rows)
    base_y = []
    for each, at in ((rows, frm % rows), (2 * MARGIN, frm % (2 * MARGIN))):
        local = at
        if each != rows:
            local = jnp.where(at < MARGIN, at + start_a, at - MARGIN + start_b)
        world = local + band_rank * rows
        fits = (to // rows == frm // each) & (world >= 0) & (world < height)
        base_y.append(jnp.where(fits, local - to % rows + CENTER, FAR))
    for j in range(2):
        for i in range(0, lanes, 16):
            for v in range(VIEWS):
                for s in range(slab):
                    row = taps[1][v * slab + s : v * slab + s + 1]
                    filter_y[v, s, i : i + 16, j * lanes : (j + 1) * lanes] = lane_pick(
                        row, base_y[j][i : i + 16]
                    ).astype(jnp.bfloat16)

    shape = filter_w.shape
    half = shape[1] // VIEWS
    column = iota(shape, 0)
    local = iota(shape, 1) % half - MARGIN
    q = jnp.where(iota(shape, 1) < half, tables[5:6, 2:3], tables[6:7, 2:3])
    num = q * (2 * (depth_rank * strip + column) + 1 - width) + width
    whole = num // (2 * width)
    frac = (num - whole * (2 * width)).astype(jnp.float32) / (2.0 * width)
    filter_w[...] = lanczos(frac - (local - column - whole).astype(jnp.float32))


def slab_kernel(
    tables, palette, filter_x, filter_y, own, got_a, got_b, keep, send, classed, near, params, sem
):
    scalars = pltpu.make_async_copy(tables, params, sem)
    scalars.start()
    slab = own.shape[1]
    lanes, width = own.shape[2:]
    rows = lanes // 4
    fill = 8 * MARGIN
    codes_a = got_a[...].astype(jnp.int32)
    codes_b = got_b[...].astype(jnp.int32)
    for s in range(slab):
        for v in range(VIEWS):
            near[v, s, fill:] = jnp.zeros((lanes - fill, width), jnp.bfloat16)

        def store(v, k, part):
            near[v, s, :fill, k * LANES : (k + 1) * LANES] = part

        at = slice(s * MARGIN, (s + 1) * MARGIN)
        voxels = jnp.concatenate([codes_a[at], codes_b[at]], axis=0)
        shear_columns(voxels, palette[...], filter_x[s], classed, store)
    scalars.wait()
    chunk = 2 * LANES
    for v in range(VIEWS):
        facing = params[5 + v, 3] >= 0
        for side in (slice(0, HALO), slice(HALO + width, 2 * HALO + width)):
            keep[v, side] = jnp.zeros((HALO, lanes), jnp.float32)
            send[v, side] = jnp.zeros((HALO, lanes), jnp.bfloat16)
        for k in range(width // chunk):
            for step in range(slab):
                s = jnp.where(facing, step, slab - 1 - step)
                source = jnp.concatenate(
                    [
                        own[v, s, :, k * chunk : (k + 1) * chunk],
                        near[v, s, :, k * chunk : (k + 1) * chunk],
                    ],
                    axis=0,
                )
                sheared = jnp.dot(filter_y[v, s], source, preferred_element_type=jnp.float32)
                if step == 0:
                    picture = sheared
                    continue
                through = 1.0 - picture[3 * rows :]
                picture = picture + jnp.concatenate([through] * 4, axis=0) * sheared
            turned = picture.T
            at = slice(HALO + k * chunk, HALO + (k + 1) * chunk)
            keep[v, at] = turned
            send[v, at] = turned.astype(jnp.bfloat16)


def merge_kernel(tables, keep, got, out):
    strips, both, lanes = out.shape
    span = both // VIEWS
    wide = span + 2 * (HALO - MARGIN)
    rows = lanes // 4
    shape = (wide, lanes)
    core = jnp.broadcast_to(tables[4:5, 0:1] % 2, shape)
    second = core == 1
    pick = 3 * rows + iota(shape, 1) % rows
    forward = [
        jnp.broadcast_to((tables[5 + v : 6 + v, 3:4] >= 0).astype(jnp.int32), shape)
        for v in range(VIEWS)
    ]
    for k in range(strips):
        low = slice(k * wide, (k + 1) * wide)
        high = slice(k * wide + wide // 2, (k + 1) * wide + wide // 2)
        done = []
        for v in range(VIEWS):
            mine_front = forward[v] + core == 1
            mine = jnp.where(second, keep[v, high], keep[v, low])
            other = jnp.where(second, got[v, high], got[v, low]).astype(jnp.float32)
            front = jnp.where(mine_front, mine, other)
            back = jnp.where(mine_front, other, mine)
            merged = front + (1.0 - lane_gather(front, pick)) * back
            done.append(merged[HALO - MARGIN : HALO - MARGIN + span])
        out[k] = jnp.concatenate(done, axis=0).astype(jnp.bfloat16)


def final_kernel(tables, filter_w, arrived, out):
    slabs, both, lanes = arrived.shape
    span = both // VIEWS
    rows = lanes // 4
    pick = 3 * rows + iota((span, lanes), 1) % rows
    for v in range(VIEWS):
        facing = jnp.broadcast_to(tables[5 + v : 6 + v, 3:4], (both, lanes)) >= 0
        picture = jnp.zeros((span, lanes), jnp.float32)
        through = jnp.ones((span, lanes), jnp.float32)
        for k in range(slabs):
            ahead = arrived[k].astype(jnp.float32)
            behind = arrived[slabs - 1 - k].astype(jnp.float32)
            part = jnp.where(facing, ahead, behind)[v * span : (v + 1) * span]
            picture = picture + through * part
            through = through * (
                1.0 - lane_gather(part, pick)
            )
        half = filter_w.shape[1] // VIEWS
        final = jnp.dot(
            filter_w[:, v * half : v * half + span],
            picture,
            precision=lax.Precision.HIGHEST,
            preferred_element_type=jnp.float32,
        )
        for c in range(4):
            out[v, :, c, :] = final[:, c * rows : (c + 1) * rows]


def call(kernel, outs, scratch=(), spaces=(), out_spaces=None):
    def run(*args):
        given = list(spaces) + [pltpu.VMEM] * (len(args) - len(spaces))
        where = out_spaces or jax.tree.map(lambda _: pltpu.VMEM, outs)
        return pl.pallas_call(
            kernel,
            out_shape=outs,
            in_specs=[pl.BlockSpec(memory_space=space) for space in given],
            out_specs=jax.tree.map(lambda space: pl.BlockSpec(memory_space=space), where),
            scratch_shapes=list(scratch),
            compiler_params=pltpu.CompilerParams(vmem_limit_bytes=VMEM_LIMIT),
        )(*args)

    return run


def body(volume, tf_table, view_code):
    slab, rows, width = volume.shape
    depth_size = lax.axis_size("depth")
    band_size = lax.axis_size("band")
    strip = width // depth_size
    lanes = 4 * rows
    bf16, f32, i32 = jnp.bfloat16, jnp.float32, jnp.int32
    shape = jax.ShapeDtypeStruct
    smem = (pltpu.SMEM,)
    ids = jnp.stack(
        [lax.axis_index("depth"), lax.axis_index("band"), jnp.int32(depth_size), jnp.int32(band_size)]
    ).astype(i32)
    wide = tf_table.shape[1]
    tables = jnp.concatenate(
        [tf_table]
        + [jnp.pad(part, ((0, 0), (0, wide - 4))) for part in (ids[None], view_code)]
        + [jnp.zeros((1, wide), i32)],
        axis=0,
    )
    voxels = volume.astype(bf16)
    even = lax.axis_index("band") % 2 == 0
    first = voxels[:, :MARGIN].reshape(slab * MARGIN, width)
    last = voxels[:, rows - MARGIN :].reshape(slab * MARGIN, width)
    send_a = jnp.where(even, last, first)
    send_b = jnp.where(even, first, last)
    got_a = lax.ppermute(send_a, "band", pairs(band_size, 0))
    got_b = lax.ppermute(send_b, "band", pairs(band_size, 1))
    palette, own, filter_x, filter_y, filter_w = call(
        functools.partial(own_kernel, slab * depth_size, rows * band_size),
        (
            shape(tf_table.shape, f32),
            shape((VIEWS, slab, lanes, width), bf16),
            shape((slab, 2 * LANES, VIEWS * LANES), bf16),
            shape((VIEWS, slab, lanes, 2 * lanes), bf16),
            shape((strip, VIEWS * (strip + 2 * HALO)), f32),
        ),
        (pltpu.VMEM((lanes, width + LANES), bf16),),
    )(tables, voxels)
    padded = (VIEWS, width + 2 * HALO, lanes)
    keep, send = call(
        slab_kernel,
        (shape(padded, f32), shape(padded, bf16)),
        (
            pltpu.VMEM((8 * MARGIN, width + LANES), bf16),
            pltpu.VMEM((VIEWS, slab, lanes, width), bf16),
            pltpu.SMEM(tables.shape, i32),
            pltpu.SemaphoreType.DMA(()),
        ),
        (pl.ANY,),
    )(tables, palette, filter_x, filter_y, own, got_a, got_b)
    got = lax.ppermute(send, "depth", pairs(depth_size, 0))
    merged = shape((depth_size // 2, VIEWS * (strip + 2 * MARGIN), lanes), bf16)
    merged = call(merge_kernel, merged)(tables, keep, got)
    arrived = lax.all_to_all(
        merged,
        "depth",
        split_axis=0,
        concat_axis=0,
        tiled=True,
        axis_index_groups=[list(range(i, depth_size, 2)) for i in range(2)],
    )
    final = shape((VIEWS, strip, 4, rows), f32)
    return call(final_kernel, final)(tables, filter_w, arrived)


def solution(mesh):
    placed = (P("depth", "band", None), P(), P())
    return jax.shard_map(
        body, mesh=mesh, in_specs=placed, out_specs=P(None, "depth", None, "band"), check_vma=False
    )
```
